128 devices in a mesh: row: 8 (over y_hi, x), col: 16 (over y_lo, z, core).
Axes of the slice: x: 4, y: 4 (y_hi: 2, y_lo: 2; y = y_hi * 2 + y_lo), z: 4, core: 2. Of those that a mesh axis runs over, the one named last changes fastest.
Arguments:
- front_matrix: float32 [8, 8, 256, 4, 16, 256], P(None, 'row', None, None, 'col'), may hold values from -6 to 6
- swap_rows: int32 [3, 256], replicated, may hold values from 0 to 16383, as said below
- l_inverse: float32 [3, 256, 256], replicated, may hold values from -1 to 1, as said below
- u_inverse: float32 [3, 256, 256], replicated, may hold values from -1 to 1, as said below
- contrib_tiles: float32 [12288, 128, 128], P(('row', 'col')), may hold values from -6 to 6
- tile_owner: int32 [12288, 1], P(('row', 'col')), may hold values from 0 to 127; in each aligned block of 96 rows (0 to 95, 96 to 191, ...) at most 2 rows name the same one
- tile_spot: int32 [12288], P(('row', 'col')), may hold values from 0 to 127
Outputs:
- factored: float32 [8, 8, 256, 4, 16, 256], P(None, 'row', None, None, 'col')
The draws below stay inside these ranges and needn't reach their ends.
Inputs may be any that keep to these rules, and one draw needn't show every extreme that they name: For every k and j, swap_rows[k, j] is either k * 256 + j or a row of (k + 1) * 256 or more; within one k the entries of the second kind are distinct. Each l_inverse[k] is unit lower triangular. Each u_inverse[k] is upper triangular with a positive diagonal. `tile_owner`: among the 96 tiles held by one device, at most 2 have the same owner; some device's tiles reach that bound.
All inputs are finite; a program needn't handle non-finite values.
Results may differ from the reference program's by a relative error of at most 0.00015.
Values sent between devices are 32-bit elements; how exact they have to be, the bound alone decides.
No kernel may reach another device: no remote copies, remote signals or barrier semaphores. Data moves between devices by JAX's collectives and lax.ppermute only.
A program may use at most 192 MiB of HBM per device.

```python
import math
import jax
import jax.numpy as jnp
import numpy as np
from jax import lax

ORDER = 16384
NB = 256
TILE = 128
STEPS = 3
CAP = 2
TILES_DEV = 96
COLS_DEV = 1024
BR = 8
BC = 4
LOCAL_TILES = 128
TILES = 12288
N_ROW = 8
N_COL = 16
DEVICES = 128


def draw_swap_rows(key, part):
    chosen_rows = []
    for window_step in range(STEPS):
        past_row = (window_step + 1) * NB
        step_key = jax.random.fold_in(key, window_step + 11)
        shuffled = jax.random.permutation(step_key, ORDER - past_row)[:NB] + past_row
        staying = jax.random.randint(jax.random.fold_in(step_key, 7), (NB,), 0, 4) == 0
        home_rows = window_step * NB + jnp.arange(NB)
        chosen_rows.append(jnp.where(staying, home_rows, shuffled).astype(jnp.int32))
    return jnp.stack(chosen_rows)


def draw_l_inverse(key, part):
    spread_scale = (0.5 / NB) ** 0.5
    step_key = jax.random.fold_in(key, 23)
    entries = jax.random.normal(step_key, (STEPS, NB, NB), jnp.float32) * spread_scale
    factor = jnp.tril(entries, -1) + jnp.eye(NB, dtype=jnp.float32)
    return jnp.clip(factor, -1.0, 1.0)


def draw_u_inverse(key, part):
    off_key = jax.random.fold_in(key, 37)
    diag_key = jax.random.fold_in(key, 41)
    entries = jax.random.normal(off_key, (STEPS, NB, NB), jnp.float32) * 0.5 / NB
    diagonal = jnp.exp(jax.random.uniform(diag_key, (STEPS, NB), jnp.float32, -0.7, 0.7)) / NB ** 0.5
    factor = jnp.triu(entries, 1) + diagonal[:, :, None] * jnp.eye(NB, dtype=jnp.float32)
    return jnp.clip(factor, -1.0, 1.0)


def set_ends(drawn, rng, smallest, top_value):
    place = [jax.random.randint(jax.random.fold_in(rng, axis), (), 0, length) for axis, length in enumerate(drawn.shape)]
    longest = drawn.shape.index(max(drawn.shape))
    neighbour = place[:longest] + [(place[longest] + 1) % drawn.shape[longest]] + place[longest + 1:]
    return drawn.at[tuple(place)].set(smallest).at[tuple(neighbour)].set(top_value)


def level_of(rng, shape, split, smallest, top_value):
    def one(axis_at, parts):
        steps = jax.random.uniform(jax.random.fold_in(jax.random.fold_in(rng, 6), axis_at), (parts,), jnp.float32, smallest / len(split), top_value / len(split))
        return jnp.repeat(jnp.exp(steps), shape[axis_at] // parts).reshape((-1,) + (1,) * (len(shape) - axis_at - 1))

    factor_of = one(*split[0])
    for cut in split[1:]:
        factor_of = factor_of * one(*cut)
    return factor_of


def deal_out(key, own, number, rows, count, top, bound, lean):
    sequence = jax.random.permutation(key, count)
    heavy_load, common = portions_of(count, rows * top, bound, lean, True), portions_of(count, rows * top, bound, lean, False)
    places = jnp.arange(count)

    def named(lengths, rotation):
        used = int((lengths > 0).sum())
        fixed = max(1, used // 4)
        shifted = fixed + (places - fixed + rotation * (used - fixed)) % max(1, count - fixed)
        return jnp.zeros((count,), jnp.int32).at[sequence[jnp.where(places < fixed, places, shifted)]].set(jnp.asarray(lengths, jnp.int32))

    lengths = jnp.where(number % 4 == 0, named(heavy_load, number // 4), named(common, number - number // 4 - 1))
    mixed = jax.random.permutation(jax.random.fold_in(own, 3), count)
    donor, receiver = mixed[0:count // 2 * 2:2], mixed[1:count // 2 * 2:2]
    margin = jnp.minimum(lengths[donor] - 1, bound - lengths[receiver]) // 2
    margin = jnp.where((donor == sequence[0]) | (receiver == sequence[0]) | (lengths[receiver] == 0), 0, jnp.maximum(margin, 0))
    shifted = jax.random.randint(jax.random.fold_in(own, 4), (count // 2,), 0, 1 << 20) % (margin + 1)
    lengths = lengths.at[donor].add(-shifted).at[receiver].add(shifted)
    labels = jnp.searchsorted(jnp.cumsum(lengths), jnp.arange(rows * top), side="right").astype(jnp.int32)
    table = labels.reshape(top, rows).T
    table = table[jax.random.permutation(jax.random.fold_in(own, 1), rows)]
    rotation = jax.random.randint(jax.random.fold_in(own, 2), (rows, 1), 0, top)
    return jnp.take_along_axis(table, (jnp.arange(top)[None, :] + rotation) % top, axis=1)


def portions_of(count, total, reach, skew, full):
    loads = [(1 << 20) // math.isqrt(grade ** skew) + 1 for grade in range(1, count + 1)]
    largest = reach if full else min(reach, max(-(-total // count), total * loads[0] // sum(loads)))
    least = 1 if total - largest >= count - 1 else 0
    given, spare = [largest] + [least] * (count - 1), total - largest - least * (count - 1)
    while spare > 0:
        free = [i for i in range(1, count) if given[i] < largest] or [i for i in range(1, count) if given[i] < reach]
        pool, budget = sum([loads[i] for i in free]), spare
        for i in free:
            extra = min(reach - given[i], max(1, budget * loads[i] // pool), spare)
            given[i] = given[i] + extra
            spare = spare - extra
    return np.array(given)


def scatter_about(own_key, extent, width, most, shards=(), held_as=jnp.bfloat16):
    result = width * jax.random.normal(own_key, extent, jnp.float32)
    if shards:
        result = result * level_of(own_key, extent, shards, -0.22, 0.18)
    return jnp.clip(result, -most, most).astype(held_as)


def setup_inputs(seed: int = 0) -> dict:
    splits = jax.random.split(jax.random.key(seed), 8)
    front_matrix = scatter_about(splits[0], (BR, N_ROW, NB, BC, N_COL, NB), 1.0, 6.0, ((1, 8), (4, 16)), jnp.float32)
    swap_rows = draw_swap_rows(jax.random.fold_in(splits[7], 71), 0)
    l_inverse = draw_l_inverse(jax.random.fold_in(splits[7], 71), 0)
    u_inverse = draw_u_inverse(jax.random.fold_in(splits[7], 71), 0)
    contrib_tiles = scatter_about(splits[4], (TILES, TILE, TILE), 1.0, 6.0, ((0, 128),), jnp.float32)
    tile_owner_keys = jax.random.split(jax.random.fold_in(splits[5], 1), TILES // TILES_DEV)
    tile_owner_turns = jax.random.permutation(jax.random.fold_in(splits[5], 3), TILES // TILES_DEV)
    tile_owner = jax.vmap(lambda own, number: deal_out(jax.random.fold_in(splits[5], 2), own, number, TILES_DEV, DEVICES, 1, CAP, 2))(tile_owner_keys, tile_owner_turns).reshape((TILES, 1))
    tile_spot = set_ends(jax.random.randint(splits[6], (TILES,), 0, LOCAL_TILES), jax.random.fold_in(splits[6], 1), 0, LOCAL_TILES - 1).astype(jnp.int32)
    return {"front_matrix": front_matrix, "swap_rows": swap_rows, "l_inverse": l_inverse, "u_inverse": u_inverse, "contrib_tiles": contrib_tiles, "tile_owner": tile_owner, "tile_spot": tile_spot}


def reference(front_matrix, swap_rows, l_inverse, u_inverse, contrib_tiles, tile_owner, tile_spot):
    precise = lax.Precision.HIGHEST
    matrix = front_matrix.reshape(ORDER, ORDER)
    all_rows = jnp.arange(ORDER, dtype=jnp.int32)
    for window_step in range(STEPS):
        start_row = window_step * NB
        past_row = start_row + NB
        targets = swap_rows[window_step].astype(jnp.int32)
        home_rows = (start_row + jnp.arange(NB, dtype=jnp.int32)).astype(jnp.int32)
        row_order = all_rows.at[home_rows].set(targets).at[targets].set(home_rows)
        matrix = matrix[row_order]
        lower_part = jnp.dot(matrix[past_row:, start_row:past_row], u_inverse[window_step], precision=precise, preferred_element_type=jnp.float32)
        upper_part = jnp.dot(l_inverse[window_step], matrix[start_row:past_row, past_row:], precision=precise, preferred_element_type=jnp.float32)
        matrix = matrix.at[past_row:, start_row:past_row].set(lower_part)
        matrix = matrix.at[start_row:past_row, past_row:].set(upper_part)
        update = jnp.dot(lower_part, upper_part, precision=precise, preferred_element_type=jnp.float32)
        matrix = matrix.at[past_row:, past_row:].add(-update)
    owners = tile_owner[:, 0].astype(jnp.int32)
    owner_row = owners // N_COL
    owner_col = owners % N_COL
    col_tiles = COLS_DEV // TILE
    local_row = (tile_spot // col_tiles) * TILE
    local_col = (tile_spot % col_tiles) * TILE
    global_row = ((local_row // NB) * N_ROW + owner_row) * NB + local_row % NB
    global_col = ((local_col // NB) * N_COL + owner_col) * NB + local_col % NB
    blocks = matrix.reshape(ORDER // TILE, TILE, ORDER // TILE, TILE)
    blocks = blocks.at[(global_row // TILE).astype(jnp.int32), :, (global_col // TILE).astype(jnp.int32), :].add(contrib_tiles)
    return blocks.reshape(BR, N_ROW, NB, BC, N_COL, NB)
```

```python
import jax
import jax.numpy as jnp
from jax import lax
from jax.experimental import pallas as pl
from jax.experimental.pallas import tpu as pltpu
from jax.sharding import PartitionSpec as P

STEPS = 3
CAP = 2
NB = 256
LANES = 128
GROUPS = 8
F32 = jnp.float32
BF16 = jnp.bfloat16
I32 = jnp.int32
ANY = pl.BlockSpec(memory_space=pl.ANY)
SMEM = pl.BlockSpec(memory_space=pltpu.SMEM)
BIG = pltpu.CompilerParams(vmem_limit_bytes=60 * 1024 * 1024)


def halves(x):
    high = x.astype(BF16)
    return high, (x - high.astype(F32)).astype(BF16)


def product(a, b):
    def one(x, y):
        return jnp.dot(x, y, preferred_element_type=F32)

    return one(a[0], b[0]) + (one(a[0], b[1]) + one(a[1], b[0]))


def pack_body(owner, spot, tiles, send, ids, seen, sem):
    count = tiles.shape[0]

    def clear(i, carry):
        ids[i] = -1
        return carry

    def fresh(i, carry):
        seen[i] = 0
        return carry

    lax.fori_loop(0, ids.shape[0], clear, 0)
    lax.fori_loop(0, seen.shape[0], fresh, 0)

    def put(i, carry):
        d = owner[i]
        rank = seen[d]
        seen[d] = rank + 1
        slot = d * CAP + rank
        ids[slot] = spot[i]
        pltpu.make_async_copy(tiles.at[i], send.at[slot], sem).start()
        return carry

    lax.fori_loop(0, count, put, 0)
    pltpu.make_async_copy(tiles, send.at[pl.ds(0, count)], sem).wait()


def pack(tiles, owner, spot, devices):
    edge = tiles.shape[1]
    return pl.pallas_call(
        pack_body,
        in_specs=[SMEM, SMEM, ANY],
        out_specs=[ANY, SMEM],
        out_shape=[
            jax.ShapeDtypeStruct((devices * CAP, edge, edge), F32),
            jax.ShapeDtypeStruct((devices * CAP,), I32),
        ],
        scratch_shapes=[pltpu.SMEM((devices,), I32), pltpu.SemaphoreType.DMA(())],
        name="pack_tiles",
    )(owner, spot, tiles)


def pick_body(place, rows, out, sem):
    out[...] = jnp.zeros_like(out)

    def go(i, n):
        at = place[i]

        @pl.when(at >= 0)
        def _():
            pltpu.make_async_copy(rows.at[at], out.at[i], sem).start()

        return n + (at >= 0).astype(I32)

    started = lax.fori_loop(0, place.shape[0], go, 0)

    def finish(i, carry):
        pltpu.make_async_copy(rows.at[0], out.at[0], sem).wait()
        return carry

    lax.fori_loop(0, started, finish, 0)


def pick(place, rows):
    count = place.shape[0]
    return pl.pallas_call(
        pick_body,
        in_specs=[SMEM, ANY],
        out_specs=pl.BlockSpec(memory_space=pltpu.VMEM),
        out_shape=jax.ShapeDtypeStruct((count, GROUPS, LANES), F32),
        scratch_shapes=[pltpu.SemaphoreType.DMA(())],
        compiler_params=BIG,
        name="pick_rows",
    )(place, rows)


def land_body(me, land, old, block, *rest):
    sources, (out, at, what, total, sem) = rest[:-5], rest[-5:]
    step = pl.program_id(0)
    height = block.shape[0]

    @pl.when(step == 0)
    def _():
        def note(i, n):
            at[n] = land[i]
            what[n] = old[i]
            return n + (land[i] >= 0).astype(I32)

        total[0] = lax.fori_loop(0, land.shape[0], note, 0)

    out[...] = block[...]
    first = step * height

    def go(i, n):
        row = at[i] - first
        inside = (row >= 0) & (row < height)

        @pl.when(inside)
        def _():
            home = what[i] // NB
            turn = lax.rem(me[0] - home + len(sources), len(sources))
            for t, source in enumerate(sources):

                @pl.when(turn == t)
                def _():
                    pltpu.make_async_copy(source.at[lax.rem(what[i], NB)], out.at[row], sem).start()

        return n + inside.astype(I32)

    started = lax.fori_loop(0, total[0], go, 0)

    def finish(i, carry):
        pltpu.make_async_copy(sources[0].at[0], out.at[0], sem).wait()
        return carry

    lax.fori_loop(0, started, finish, 0)


def land_rows(me, land, old, rows, sources):
    height = NB
    slab = pl.BlockSpec((height, GROUPS, LANES), lambda i: (i, 0, 0))
    events = land.shape[0]
    return pl.pallas_call(
        land_body,
        grid=(rows.shape[0] // height,),
        in_specs=[SMEM, SMEM, SMEM, slab] + [ANY] * len(sources),
        out_specs=slab,
        out_shape=jax.ShapeDtypeStruct(rows.shape, F32),
        scratch_shapes=[
            pltpu.SMEM((events + 1,), I32),
            pltpu.SMEM((events + 1,), I32),
            pltpu.SMEM((1,), I32),
            pltpu.SemaphoreType.DMA(()),
        ],
        compiler_params=BIG,
        name="land_rows",
    )(me, land, old, rows, *sources)


def panel_body(me, block, top, corner, out):
    step = pl.program_id(0)
    height = block.shape[0]
    for g in range(2):
        out[0, :height, g * LANES : (g + 1) * LANES] = block[:, g, :]
        out[0, height:, g * LANES : (g + 1) * LANES] = corner[:, g, :]

    @pl.when((step * height < NB) & (me[0] < STEPS))
    def _():
        for g in range(2):
            out[0, :height, g * LANES : (g + 1) * LANES] = top[:, g, :]


def panel(me, rows, chosen, parts):
    height = rows.shape[0] // parts
    share = chosen.shape[0] // parts
    per = NB // height

    def top_at(i, me):
        return (jnp.minimum(me[0], STEPS - 1) * per + jnp.minimum(i, per - 1), 0, 0)

    return pl.pallas_call(
        panel_body,
        grid_spec=pltpu.PrefetchScalarGridSpec(
            num_scalar_prefetch=1,
            grid=(parts,),
            in_specs=[
                pl.BlockSpec((height, GROUPS, LANES), lambda i, me: (i, 0, 0)),
                pl.BlockSpec((height, GROUPS, LANES), top_at),
                pl.BlockSpec((share, GROUPS, LANES), lambda i, me: (i, 0, 0)),
            ],
            out_specs=pl.BlockSpec((1, height + share, NB), lambda i, me: (i, 0, 0)),
        ),
        out_shape=jax.ShapeDtypeStruct((parts, height + share, NB), F32),
        compiler_params=BIG,
        name="panel_parts",
    )(me, rows, chosen, chosen)


def main_body(me, linv, uinv, chosen, gathered, panels, block, out, corner, final, upper, upper_hi, upper_lo, factor, sem):
    step = pl.program_id(0)
    parts, _, share, _ = corner.shape
    full = parts * share
    height = gathered.shape[2] - share

    def ui(k):
        return halves(uinv[k])

    @pl.when(step == 0)
    def _():
        copy = pltpu.make_async_copy(gathered.at[:, :, pl.ds(height, share), :], corner, sem)
        copy.start()
        copy.wait()
        cols = [corner[:, k].reshape(full, NB) for k in range(STEPS)]
        n = [[cols[k][i * NB : (i + 1) * NB] for k in range(STEPS)] for i in range(STEPS)]
        low = {}
        for k in range(STEPS):
            x = chosen[k * NB : (k + 1) * NB].reshape(NB, GROUPS * LANES)
            for m in range(k):
                x = x - product(low[k, m], (upper_hi[m * NB : (m + 1) * NB], upper_lo[m * NB : (m + 1) * NB]))
            u = product(halves(linv[k]), halves(x))
            hi, lo = halves(u)
            upper[k * NB : (k + 1) * NB] = u
            upper_hi[k * NB : (k + 1) * NB] = hi
            upper_lo[k * NB : (k + 1) * NB] = lo
            final[k, k] = n[k][k]
            for i in range(k + 1, STEPS):
                l = product(halves(n[i][k]), ui(k))
                low[i, k] = halves(l)
                final[i, k] = l
                v = product(halves(linv[k]), halves(n[k][i]))
                final[k, i] = v
            for i in range(k + 1, STEPS):
                for j in range(k + 1, STEPS):
                    n[i][j] = n[i][j] - product(low[i, k], halves(final[k, j]))

    hi = []
    lo = []
    for k in range(STEPS):
        x = panels[:, k].reshape(2 * height, NB)
        for m in range(k):
            x = x - product((hi[m], lo[m]), halves(final[m, k]))
        l = product(halves(x), ui(k))
        factor[k] = l
        h, w = halves(l)
        hi.append(h)
        lo.append(w)
    high = jnp.concatenate(hi, axis=1)
    rest = jnp.concatenate(lo, axis=1)
    update = product((high, rest), (upper_hi[...], upper_lo[...]))
    value = block[...].reshape(2 * height, GROUPS * LANES) - update
    for s in range(2):
        for g in range(GROUPS):
            out[s, g] = value[s * height : (s + 1) * height, g * LANES : (g + 1) * LANES]
    is_top = (step == 0) & (me[0] < STEPS)

    @pl.when(is_top)
    def _():
        base = me[0] * NB
        for s in range(2):
            u = upper[pl.ds(base + s * height, height), :]
            for g in range(GROUPS):
                out[s, g] = u[:, g * LANES : (g + 1) * LANES]

    @pl.when(me[1] < STEPS)
    def _():
        for s in range(2):
            for g in range(2):
                out[s, g] = factor[me[1], s * height : (s + 1) * height, g * LANES : (g + 1) * LANES]

    @pl.when(is_top & (me[1] < STEPS))
    def _():
        for s in range(2):
            for g in range(2):
                out[s, g] = final[me[0], me[1], s * height : (s + 1) * height, g * LANES : (g + 1) * LANES]


def eliminate(me, linv, uinv, chosen, gathered, rows):
    parts, _, both, _ = gathered.shape
    share = chosen.shape[0] // parts
    height = both - share
    width = GROUPS * LANES
    whole3 = pl.BlockSpec((STEPS, NB, NB), lambda i: (0, 0, 0))
    return pl.pallas_call(
        main_body,
        grid=(parts // 2,),
        in_specs=[
            SMEM,
            whole3,
            whole3,
            pl.BlockSpec(chosen.shape, lambda i: (0, 0, 0)),
            ANY,
            pl.BlockSpec((2, STEPS, height, NB), lambda i: (i, 0, 0, 0)),
            pl.BlockSpec((2 * height, GROUPS, LANES), lambda i: (i, 0, 0)),
        ],
        out_specs=pl.BlockSpec((2, GROUPS, height, LANES), lambda i: (i, 0, 0, 0)),
        out_shape=jax.ShapeDtypeStruct((parts, GROUPS, height, LANES), F32),
        scratch_shapes=[
            pltpu.VMEM((parts, STEPS, share, NB), F32),
            pltpu.VMEM((STEPS, STEPS, NB, NB), F32),
            pltpu.VMEM((STEPS * NB, width), F32),
            pltpu.VMEM((STEPS * NB, width), BF16),
            pltpu.VMEM((STEPS * NB, width), BF16),
            pltpu.VMEM((STEPS, NB, NB), F32),
            pltpu.SemaphoreType.DMA(()),
        ],
        compiler_params=BIG,
        name="eliminate",
    )(me, linv, uinv, chosen, gathered, gathered, rows)


RING = 16


def tail_body(ids, base, received, out, acc, ring, staged, order, base_sem, ring_sem, out_sem):
    whole = pltpu.make_async_copy(base, acc, base_sem)
    whole.start()

    def note(i, n):
        order[n] = i
        return n + (ids[i] >= 0).astype(I32)

    total = lax.fori_loop(0, ids.shape[0], note, 0)

    def fetch(j):
        b = lax.rem(j, RING)
        return pltpu.make_async_copy(received.at[order[j]], ring.at[b], ring_sem.at[b])

    def prime(j, carry):
        fetch(j).start()
        return carry

    lax.fori_loop(0, jnp.minimum(total, RING), prime, 0)
    whole.wait()

    def add(j, carry):
        fetch(j).wait()
        m = ids[order[j]]
        acc[m] = acc[m] + ring[lax.rem(j, RING)]

        @pl.when(j + RING < total)
        def _():
            fetch(j + RING).start()

        return carry

    lax.fori_loop(0, total, add, 0)
    edge = acc.shape[1]
    copies = []
    for s in range(acc.shape[0] // GROUPS):
        p = s % 2
        if s >= 2:
            copies[s - 2].wait()
        for g in range(GROUPS):
            staged[p, :, g, :] = acc[s * GROUPS + g]
        copy = pltpu.make_async_copy(staged.at[p], out.at[pl.ds(s * edge, edge)], out_sem.at[p])
        copy.start()
        copies.append(copy)
    copies[-2].wait()
    copies[-1].wait()


def add_tiles(ids, base, received):
    spots, edge, _ = base.shape
    return pl.pallas_call(
        tail_body,
        in_specs=[SMEM, ANY, ANY],
        out_specs=ANY,
        out_shape=jax.ShapeDtypeStruct((spots // GROUPS * edge, GROUPS, LANES), F32),
        scratch_shapes=[
            pltpu.VMEM((spots, edge, LANES), F32),
            pltpu.VMEM((RING, edge, LANES), F32),
            pltpu.VMEM((2, edge, GROUPS, LANES), F32),
            pltpu.SMEM((ids.shape[0],), I32),
            pltpu.SemaphoreType.DMA(()),
            pltpu.SemaphoreType.DMA((RING,)),
            pltpu.SemaphoreType.DMA((2,)),
        ],
        compiler_params=BIG,
        name="add_tiles",
    )(ids, base, received)


def look(x, t, values, other):
    same = x[:, None] == t[None, :]
    hit = jnp.any(same, axis=1)
    return hit, jnp.where(hit, jnp.sum(jnp.where(same, values[None, :], 0), axis=1), other)


def permutation(swap_rows):
    t0, t1, t2 = swap_rows[0], swap_rows[1], swap_rows[2]
    j = jnp.arange(NB, dtype=I32)
    n = NB
    x = jnp.concatenate([NB + j, 2 * NB + j, t1, t2])
    _, once = look(x, t0, j, x)
    v1 = once[:n]
    y = jnp.concatenate([2 * NB + j, t2])
    _, twice = look(y, t1, v1, jnp.concatenate([once[n : 2 * n], once[3 * n :]]))
    v2 = twice[:n]
    source = jnp.concatenate([t0, once[2 * n : 3 * n], twice[n:]])
    below = STEPS * NB
    in1 = jnp.any(t0[:, None] == t1[None, :], axis=1)
    in2 = jnp.any(jnp.concatenate([t0, t1])[:, None] == t2[None, :], axis=1)
    ok0 = (t0 >= below) & ~in1 & ~in2[:n]
    ok1 = (t1 >= below) & ~in2[n:]
    ok2 = t2 >= below
    land = jnp.where(jnp.concatenate([ok0, ok1, ok2]), jnp.concatenate([t0, t1, t2]), -1)
    return source, land, jnp.concatenate([j, v1, v2])


def local(front_matrix, swap_rows, l_inverse, u_inverse, contrib_tiles, tile_owner, tile_spot):
    row_count = lax.axis_size("row")
    col_count = lax.axis_size("col")
    row_place = lax.axis_index("row").astype(I32)
    col_place = lax.axis_index("col").astype(I32)
    me = jnp.stack([row_place, col_place])
    send, ids = pack(contrib_tiles, tile_owner[:, 0], tile_spot, row_count * col_count)
    received = lax.all_to_all(send, ("row", "col"), split_axis=0, concat_axis=0, tiled=True)
    ids_in = lax.all_to_all(ids, ("row", "col"), split_axis=0, concat_axis=0, tiled=True)

    local_rows = front_matrix.shape[0] * NB
    rows = front_matrix.reshape(-1).reshape(local_rows, GROUPS, LANES)
    source, land, old = permutation(swap_rows)

    def mine(x):
        block = x // NB
        here = (block % row_count == row_place) & (x >= 0)
        return jnp.where(here, block // row_count * NB + x % NB, -1)

    chosen = lax.psum(pick(mine(source), rows), "row")
    own_top = rows[:NB]
    tops = [own_top]
    for t in range(1, row_count):
        tops.append(lax.ppermute(own_top, "row", [(p, (p + t) % row_count) for p in range(STEPS)]))
    moved = land_rows(me, mine(land), old, rows, tops)
    parts = panel(me, moved, chosen, col_count)
    dealt = lax.all_to_all(parts, "col", split_axis=0, concat_axis=0, tiled=True)[:STEPS]
    gathered = lax.all_gather(dealt.reshape(-1, NB), "col", axis=0, tiled=True)
    gathered = gathered.reshape(col_count, STEPS, -1, NB)
    base = eliminate(me, l_inverse, u_inverse, chosen, gathered, moved)
    base = base.reshape(-1, LANES, LANES)
    out = add_tiles(ids_in, base, received)
    return out.reshape(-1).reshape(front_matrix.shape)


def solution(mesh):
    placed = (
        P(None, "row", None, None, "col", None),
        P(),
        P(),
        P(),
        P(("row", "col"), None, None),
        P(("row", "col"), None),
        P(("row", "col")),
    )
    return jax.shard_map(
        local,
        mesh=mesh,
        in_specs=placed,
        out_specs=P(None, "row", None, None, "col", None),
        check_vma=False,
    )
```

```python
import jax
import jax.numpy as jnp
from jax import lax
from jax.experimental import pallas as pl
from jax.experimental.pallas import tpu as pltpu
from jax.sharding import PartitionSpec as P


STEPS = 3
CAP = 2
NB = 256
LANES = 128
GROUPS = 8
RING = 16
PARCEL = 48
F32 = jnp.float32
BF16 = jnp.bfloat16
I32 = jnp.int32
ANY = pl.BlockSpec(memory_space=pl.ANY)
SMEM = pl.BlockSpec(memory_space=pltpu.SMEM)
BIG = pltpu.CompilerParams(vmem_limit_bytes=60 * 1024 * 1024)


def halves(x):
    high = x.astype(BF16)
    return high, (x - high.astype(F32)).astype(BF16)


def product(a, b):
    def one(x, y):
        return jnp.dot(x, y, preferred_element_type=F32)

    return one(a[0], b[0]) + (one(a[0], b[1]) + one(a[1], b[0]))


def pack_body(owner, spot, tiles, *rest):
    send, ids, held, seen, load_sem, sem = rest[-6:]
    count = tiles.shape[0]
    load = pltpu.make_async_copy(tiles, held, load_sem)
    load.start()

    def clear(i, carry):
        ids[i] = -1
        return carry

    def fresh(i, carry):
        seen[i] = 0
        return carry

    lax.fori_loop(0, ids.shape[0], clear, 0)
    lax.fori_loop(0, seen.shape[0], fresh, 0)
    load.wait()

    def put(i, carry):
        d = owner[i]
        rank = seen[d]
        seen[d] = rank + 1
        slot = d * CAP + rank
        ids[slot] = spot[i]
        pltpu.make_async_copy(held.at[i], send.at[slot], sem).start()
        return carry

    lax.fori_loop(0, count, put, 0)
    pltpu.make_async_copy(held, send.at[pl.ds(0, count)], sem).wait()


def pack(tiles, owner, spot, devices):
    edge = tiles.shape[1]
    return pl.pallas_call(
        pack_body,
        in_specs=[SMEM, SMEM, ANY],
        out_specs=[ANY, SMEM],
        out_shape=[
            jax.ShapeDtypeStruct((devices * CAP, edge, edge), F32),
            jax.ShapeDtypeStruct((devices * CAP,), I32),
        ],
        scratch_shapes=[
            pltpu.VMEM(tiles.shape, F32),
            pltpu.SMEM((devices,), I32),
            pltpu.SemaphoreType.DMA(()),
            pltpu.SemaphoreType.DMA(()),
        ],
        compiler_params=BIG,
        name="pack_tiles",
    )(owner, spot, tiles)


def pick_body(place, rows, out, corner, sem):
    out[...] = jnp.zeros_like(out)

    def go(i, n):
        at = place[i]

        @pl.when(at >= 0)
        def _():
            pltpu.make_async_copy(rows.at[at], out.at[i], sem).start()

        return n + (at >= 0).astype(I32)

    started = lax.fori_loop(0, place.shape[0], go, 0)

    def finish(i, carry):
        pltpu.make_async_copy(rows.at[0], out.at[0], sem).wait()
        return carry

    lax.fori_loop(0, started, finish, 0)
    for g in range(2):
        corner[:, g * LANES : (g + 1) * LANES] = out[:, g, :]


def pick(place, rows):
    count = place.shape[0]
    vmem = pl.BlockSpec(memory_space=pltpu.VMEM)
    return pl.pallas_call(
        pick_body,
        in_specs=[SMEM, ANY],
        out_specs=[vmem, vmem],
        out_shape=[
            jax.ShapeDtypeStruct((count, GROUPS, LANES), F32),
            jax.ShapeDtypeStruct((count, NB), F32),
        ],
        scratch_shapes=[pltpu.SemaphoreType.DMA(())],
        compiler_params=BIG,
        name="pick_rows",
    )(place, rows)


def collect_body(given, out):
    total = given[0]
    for i in range(1, given.shape[0]):
        total = total + given[i]
    for i in range(out.shape[0]):
        out[i] = total


def collect(given, share):
    count = given.shape[0]
    step = 8 if share % 8 == 0 else 1
    block = pl.BlockSpec((count, share // step, GROUPS, LANES), lambda i: (0, i, 0, 0))
    return pl.pallas_call(
        collect_body,
        grid=(step,),
        in_specs=[block],
        out_specs=block,
        out_shape=jax.ShapeDtypeStruct((count, share, GROUPS, LANES), F32),
        compiler_params=BIG,
        name="collect_rows",
    )(given)


def panel_body(block, out):
    for g in range(2):
        out[0, :, g * LANES : (g + 1) * LANES] = block[:, g, :]


def panel(rows, parts):
    height = rows.shape[0] // parts
    return pl.pallas_call(
        panel_body,
        grid=(parts,),
        in_specs=[pl.BlockSpec((height, GROUPS, LANES), lambda i: (i, 0, 0))],
        out_specs=pl.BlockSpec((1, height, NB), lambda i: (i, 0, 0)),
        out_shape=jax.ShapeDtypeStruct((parts, height, NB), F32),
        compiler_params=BIG,
        name="panel_parts",
    )(rows)


def main_body(me, linv, uinv, chosen, corner, panels, block, out, leave, final, upper, upper_hi, upper_lo, factor):
    step = pl.program_id(0)
    height = panels.shape[2]

    def ui(k):
        return halves(uinv[k])

    @pl.when(step == 0)
    def _():
        cols = [corner[:, k].reshape(STEPS * NB, NB) for k in range(STEPS)]
        n = [[cols[k][i * NB : (i + 1) * NB] for k in range(STEPS)] for i in range(STEPS)]
        low = {}
        for k in range(STEPS):
            x = chosen[k * NB : (k + 1) * NB].reshape(NB, GROUPS * LANES)
            for m in range(k):
                x = x - product(low[k, m], (upper_hi[m * NB : (m + 1) * NB], upper_lo[m * NB : (m + 1) * NB]))
            u = product(halves(linv[k]), halves(x))
            hi, lo = halves(u)
            upper[k * NB : (k + 1) * NB] = u
            upper_hi[k * NB : (k + 1) * NB] = hi
            upper_lo[k * NB : (k + 1) * NB] = lo
            final[k, k] = n[k][k]
            for i in range(k + 1, STEPS):
                l = product(halves(n[i][k]), ui(k))
                low[i, k] = halves(l)
                final[i, k] = l
                v = product(halves(linv[k]), halves(n[k][i]))
                final[k, i] = v
            for i in range(k + 1, STEPS):
                for j in range(k + 1, STEPS):
                    n[i][j] = n[i][j] - product(low[i, k], halves(final[k, j]))

    hi = []
    lo = []
    for k in range(STEPS):
        x = panels[:, k].reshape(2 * height, NB)
        for m in range(k):
            x = x - product((hi[m], lo[m]), halves(final[m, k]))
        l = product(halves(x), ui(k))
        factor[k] = l
        h, w = halves(l)
        hi.append(h)
        lo.append(w)
    high = jnp.concatenate(hi, axis=1)
    rest = jnp.concatenate(lo, axis=1)
    update = product((high, rest), (upper_hi[...], upper_lo[...]))
    value = block[...].reshape(2 * height, GROUPS * LANES) - update
    for s in range(2):
        for g in range(GROUPS):
            out[s, g] = value[s * height : (s + 1) * height, g * LANES : (g + 1) * LANES]

    @pl.when(me[1] < STEPS)
    def _():
        for s in range(2):
            for g in range(2):
                out[s, g] = factor[me[1], s * height : (s + 1) * height, g * LANES : (g + 1) * LANES]

    @pl.when(step == 0)
    def _():
        for s in range(2):
            for g in range(GROUPS):
                leave[s * height : (s + 1) * height, g, :] = out[s, g]

    is_top = (step == 0) & (me[0] < STEPS)

    @pl.when(is_top)
    def _():
        base = me[0] * NB
        for s in range(2):
            u = upper[pl.ds(base + s * height, height), :]
            for g in range(GROUPS):
                out[s, g] = u[:, g * LANES : (g + 1) * LANES]

    @pl.when(is_top & (me[1] < STEPS))
    def _():
        for s in range(2):
            for g in range(2):
                out[s, g] = final[me[0], me[1], s * height : (s + 1) * height, g * LANES : (g + 1) * LANES]


def eliminate(me, linv, uinv, chosen, corner, gathered, rows):
    parts, _, height, _ = gathered.shape
    width = GROUPS * LANES
    whole3 = pl.BlockSpec((STEPS, NB, NB), lambda i: (0, 0, 0))
    return pl.pallas_call(
        main_body,
        grid=(parts // 2,),
        in_specs=[
            SMEM,
            whole3,
            whole3,
            pl.BlockSpec(chosen.shape, lambda i: (0, 0, 0)),
            pl.BlockSpec(corner.shape, lambda i: (0, 0, 0, 0)),
            pl.BlockSpec((2, STEPS, height, NB), lambda i: (i, 0, 0, 0)),
            pl.BlockSpec((2 * height, GROUPS, LANES), lambda i: (i, 0, 0)),
        ],
        out_specs=[
            pl.BlockSpec((2, GROUPS, height, LANES), lambda i: (i, 0, 0, 0)),
            pl.BlockSpec((NB, GROUPS, LANES), lambda i: (0, 0, 0)),
        ],
        out_shape=[
            jax.ShapeDtypeStruct((parts, GROUPS, height, LANES), F32),
            jax.ShapeDtypeStruct((NB, GROUPS, LANES), F32),
        ],
        scratch_shapes=[
            pltpu.VMEM((STEPS, STEPS, NB, NB), F32),
            pltpu.VMEM((STEPS * NB, width), F32),
            pltpu.VMEM((STEPS * NB, width), BF16),
            pltpu.VMEM((STEPS * NB, width), BF16),
            pltpu.VMEM((STEPS, NB, NB), F32),
        ],
        compiler_params=BIG,
        name="eliminate",
    )(me, linv, uinv, chosen, corner, gathered, rows)


def parcel_body(me, land, old, leave, *rest):
    outs, seen = rest[:-1], rest[-1]
    count = len(outs)
    for t in range(count):
        seen[t] = 0

    def go(i, carry):
        row = land[i]
        from_here = (row >= 0) & (old[i] // NB == me[0])

        @pl.when(from_here)
        def _():
            turn = lax.rem(lax.rem(row // NB, count) - me[0] + count, count)
            at = seen[turn]
            seen[turn] = at + 1
            for t, out in enumerate(outs):

                @pl.when((turn == t) & (at < out.shape[0]))
                def _():
                    out[at] = leave[lax.rem(old[i], NB)]

        return carry

    lax.fori_loop(0, land.shape[0], go, 0)


def parcel(me, land, old, leave, count):
    vmem = pl.BlockSpec(memory_space=pltpu.VMEM)
    return pl.pallas_call(
        parcel_body,
        in_specs=[SMEM, SMEM, SMEM, vmem],
        out_specs=[vmem] * count,
        out_shape=[jax.ShapeDtypeStruct((PARCEL, GROUPS, LANES), F32)] * count,
        scratch_shapes=[pltpu.SMEM((count,), I32)],
        compiler_params=BIG,
        name="parcel_rows",
    )(me, land, old, leave)


def tail_body(me, land, old, ids, base, received, *rest):
    ranked, parcels = rest[0], rest[1:-11]
    out, acc, ring, staged, order, seen, at_row, at_old, base_sem, ring_sem, out_sem = rest[-11:]
    whole = pltpu.make_async_copy(base, acc, base_sem)
    whole.start()
    count = len(parcels)
    edge = acc.shape[1]

    def note(i, n):
        order[n] = i
        return n + (ids[i] >= 0).astype(I32)

    total = lax.fori_loop(0, ids.shape[0], note, 0)

    def fetch(j):
        b = lax.rem(j, RING)
        return pltpu.make_async_copy(received.at[order[j]], ring.at[b], ring_sem.at[b])

    def prime(j, carry):
        fetch(j).start()
        return carry

    lax.fori_loop(0, jnp.minimum(total, RING), prime, 0)

    def mark(i, n):
        at_row[n] = land[i]
        at_old[n] = old[i]
        return n + ((land[i] >= 0) & (lax.rem(land[i] // NB, count) == me[0])).astype(I32)

    landed = lax.fori_loop(0, land.shape[0], mark, 0)
    for t in range(count):
        seen[t] = 0
    whole.wait()

    def settle(i, carry):
        row = at_row[i] // (NB * count) * NB + lax.rem(at_row[i], NB)
        was = at_old[i]
        turn = lax.rem(me[0] - was // NB + count, count)
        rank = seen[turn]
        seen[turn] = rank + 1
        at = jnp.minimum(rank, PARCEL - 1) if ranked is None else lax.rem(was, NB)
        spot = row // edge * GROUPS
        for t, parcel_ref in enumerate(parcels):

            @pl.when(turn == t)
            def _():
                for g in range(GROUPS):
                    acc[spot + g, pl.ds(lax.rem(row, edge), 1), :] = parcel_ref[at, pl.ds(g, 1), :]

        return carry

    lax.fori_loop(0, landed, settle, 0)

    def add(j, carry):
        fetch(j).wait()
        m = ids[order[j]]
        acc[m] = acc[m] + ring[lax.rem(j, RING)]

        @pl.when(j + RING < total)
        def _():
            fetch(j + RING).start()

        return carry

    lax.fori_loop(0, total, add, 0)
    copies = []
    for s in range(acc.shape[0] // GROUPS):
        p = s % 2
        if s >= 2:
            copies[s - 2].wait()
        for g in range(GROUPS):
            staged[p, :, g, :] = acc[s * GROUPS + g]
        copy = pltpu.make_async_copy(staged.at[p], out.at[pl.ds(s * edge, edge)], out_sem.at[p])
        copy.start()
        copies.append(copy)
    copies[-2].wait()
    copies[-1].wait()


def add_tiles(me, land, old, ids, base, received, parcels, ranked):
    spots, edge, _ = base.shape
    vmem = pl.BlockSpec(memory_space=pltpu.VMEM)
    events = land.shape[0]

    def body(me, land, old, ids, base, received, *rest):
        return tail_body(me, land, old, ids, base, received, None if ranked else True, *rest)

    return pl.pallas_call(
        body,
        in_specs=[SMEM, SMEM, SMEM, SMEM, ANY, ANY] + [vmem] * len(parcels),
        out_specs=ANY,
        out_shape=jax.ShapeDtypeStruct((spots // GROUPS * edge, GROUPS, LANES), F32),
        scratch_shapes=[
            pltpu.VMEM((spots, edge, LANES), F32),
            pltpu.VMEM((RING, edge, LANES), F32),
            pltpu.VMEM((2, edge, GROUPS, LANES), F32),
            pltpu.SMEM((ids.shape[0],), I32),
            pltpu.SMEM((len(parcels),), I32),
            pltpu.SMEM((events + 1,), I32),
            pltpu.SMEM((events + 1,), I32),
            pltpu.SemaphoreType.DMA(()),
            pltpu.SemaphoreType.DMA((RING,)),
            pltpu.SemaphoreType.DMA((2,)),
        ],
        compiler_params=BIG,
        name="add_tiles_ranked" if ranked else "add_tiles_whole",
    )(me, land, old, ids, base, received, *parcels)


def look(x, t, values, other):
    same = x[:, None] == t[None, :]
    hit = jnp.any(same, axis=1)
    return hit, jnp.where(hit, jnp.sum(jnp.where(same, values[None, :], 0), axis=1), other)


def permutation(swap_rows):
    t0, t1, t2 = swap_rows[0], swap_rows[1], swap_rows[2]
    j = jnp.arange(NB, dtype=I32)
    n = NB
    x = jnp.concatenate([NB + j, 2 * NB + j, t1, t2])
    _, once = look(x, t0, j, x)
    v1 = once[:n]
    y = jnp.concatenate([2 * NB + j, t2])
    _, twice = look(y, t1, v1, jnp.concatenate([once[n : 2 * n], once[3 * n :]]))
    v2 = twice[:n]
    source = jnp.concatenate([t0, once[2 * n : 3 * n], twice[n:]])
    below = STEPS * NB
    in1 = jnp.any(t0[:, None] == t1[None, :], axis=1)
    in2 = jnp.any(jnp.concatenate([t0, t1])[:, None] == t2[None, :], axis=1)
    ok0 = (t0 >= below) & ~in1 & ~in2[:n]
    ok1 = (t1 >= below) & ~in2[n:]
    ok2 = t2 >= below
    land = jnp.where(jnp.concatenate([ok0, ok1, ok2]), jnp.concatenate([t0, t1, t2]), -1)
    return source, land, jnp.concatenate([j, v1, v2])


def step(front_matrix, swap_rows, l_inverse, u_inverse, contrib_tiles, tile_owner, tile_spot):
    row_count = lax.axis_size("row")
    col_count = lax.axis_size("col")
    row_place = lax.axis_index("row").astype(I32)
    col_place = lax.axis_index("col").astype(I32)
    me = jnp.stack([row_place, col_place])
    local_rows = front_matrix.shape[0] * NB
    rows = front_matrix.reshape(-1).reshape(local_rows, GROUPS, LANES)

    def exchange(x, axes):
        return lax.all_to_all(x, axes, split_axis=0, concat_axis=0, tiled=True)

    parts = panel(rows, col_count)
    dealt = exchange(parts, "col")
    swap_rows, parts = lax.optimization_barrier((swap_rows, parts))
    source, land, old = permutation(swap_rows)
    block = source // NB
    place = jnp.where(block % row_count == row_place, block // row_count * NB + source % NB, -1)
    send, ids = pack(contrib_tiles, tile_owner[:, 0], tile_spot, row_count * col_count)
    share = place.shape[0] // row_count
    place = jnp.pad(place.reshape(row_count, share), ((0, 0), (0, 1)), constant_values=-1)
    picked, corner = pick(place.reshape(-1), rows)
    notes = ids.astype(F32).reshape(row_count, col_count, CAP).transpose(1, 0, 2).reshape(col_count, -1)
    notes = jnp.pad(notes[:, None, :], ((0, 0), (0, 7), (0, NB - notes.shape[1])))
    corner = corner.reshape(row_count, share + 1, NB)[:, :share].reshape(col_count, -1, NB)
    corner = jnp.concatenate([corner, notes], axis=1)
    corner, dealt = lax.optimization_barrier((corner, dealt))
    corner = exchange(corner, "col")
    notes = corner[:, -8, : row_count * CAP].reshape(col_count, row_count, CAP).transpose(1, 0, 2)
    notes = notes.reshape(row_count, -1)
    notes = jnp.pad(notes, ((0, 0), (0, GROUPS * LANES - notes.shape[1]))).reshape(-1, 1, GROUPS, LANES)
    picked = picked.reshape(row_count, share + 1, GROUPS, LANES)
    picked = lax.dynamic_update_slice(picked, notes, (0, share, 0, 0))
    given = exchange(picked, "row")
    ids_in = given[:, share].reshape(row_count, -1)[:, : col_count * CAP].reshape(-1).astype(I32)
    gathered = lax.all_gather(dealt[:STEPS].reshape(-1, NB), "col", axis=0, tiled=True)
    gathered = gathered.reshape(col_count, STEPS, -1, NB)
    corner, given = lax.optimization_barrier((corner, given))
    corner = lax.psum(corner[:STEPS, :-8], "row").reshape(-1, NB)
    corner = lax.all_gather(corner, "col", axis=0, tiled=True).reshape(col_count, STEPS, -1, NB)
    summed = collect(given, share)
    chosen = exchange(summed, "row")
    chosen = chosen.reshape(-1, GROUPS, LANES)
    send, chosen, corner, gathered = lax.optimization_barrier((send, chosen, corner, gathered))
    received = exchange(send, ("row", "col"))

    base, leave = eliminate(me, l_inverse, u_inverse, chosen, corner, gathered, rows)
    base = base.reshape(-1, LANES, LANES)

    def shift(x, t):
        return lax.ppermute(x, "row", [(p, (p + t) % row_count) for p in range(STEPS)])

    parcels = parcel(me, land, old, leave, row_count)
    parcels = [parcels[0]] + [shift(parcels[t], t) for t in range(1, row_count)]
    pair = jnp.where(land >= 0, old // NB * row_count + land // NB % row_count, -1)
    loads = jnp.sum((pair[:, None] == jnp.arange(STEPS * row_count, dtype=I32)[None, :]).astype(I32), axis=0)

    def ranked(parcels, leave):
        return add_tiles(me, land, old, ids_in, base, received, parcels, True)

    def whole(parcels, leave):
        every = [leave] + [shift(leave, t) for t in range(1, row_count)]
        return add_tiles(me, land, old, ids_in, base, received, every, False)

    out = lax.cond(jnp.max(loads) > PARCEL, whole, ranked, parcels, leave)
    return out.reshape(-1).reshape(front_matrix.shape)


def solution(mesh):
    placed = (
        P(None, "row", None, None, "col", None),
        P(),
        P(),
        P(),
        P(("row", "col"), None, None),
        P(("row", "col"), None),
        P(("row", "col")),
    )
    return jax.shard_map(
        step,
        mesh=mesh,
        in_specs=placed,
        out_specs=P(None, "row", None, None, "col", None),
        check_vma=False,
    )
```

```python
import jax
import jax.numpy as jnp
from jax import lax
from jax.experimental import pallas as pl
from jax.experimental.pallas import tpu as pltpu
from jax.sharding import PartitionSpec as P


STEPS = 3
CAP = 2
NB = 256
LANES = 128
GROUPS = 8
RING = 16
PARCEL = 48
F32 = jnp.float32
BF16 = jnp.bfloat16
I32 = jnp.int32
ANY = pl.BlockSpec(memory_space=pl.ANY)
SMEM = pl.BlockSpec(memory_space=pltpu.SMEM)
BIG = pltpu.CompilerParams(vmem_limit_bytes=60 * 1024 * 1024)


def halves(x):
    high = x.astype(BF16)
    return high, (x - high.astype(F32)).astype(BF16)


def product(a, b):
    def one(x, y):
        return jnp.dot(x, y, preferred_element_type=F32)

    return one(a[0], b[0]) + (one(a[0], b[1]) + one(a[1], b[0]))


def pack_body(owner, spot, tiles, *rest):
    send, ids, held, seen, load_sem, sem = rest[-6:]
    count = tiles.shape[0]
    load = pltpu.make_async_copy(tiles, held, load_sem)
    load.start()

    def clear(i, carry):
        ids[i] = -1
        return carry

    def fresh(i, carry):
        seen[i] = 0
        return carry

    lax.fori_loop(0, ids.shape[0], clear, 0)
    lax.fori_loop(0, seen.shape[0], fresh, 0)
    load.wait()

    def put(i, carry):
        d = owner[i]
        rank = seen[d]
        seen[d] = rank + 1
        slot = d * CAP + rank
        ids[slot] = spot[i]
        pltpu.make_async_copy(held.at[i], send.at[slot], sem).start()
        return carry

    lax.fori_loop(0, count, put, 0)
    pltpu.make_async_copy(held, send.at[pl.ds(0, count)], sem).wait()


def pack(tiles, owner, spot, devices):
    edge = tiles.shape[1]
    return pl.pallas_call(
        pack_body,
        in_specs=[SMEM, SMEM, ANY],
        out_specs=[ANY, SMEM],
        out_shape=[
            jax.ShapeDtypeStruct((devices * CAP, edge, edge), F32),
            jax.ShapeDtypeStruct((devices * CAP,), I32),
        ],
        scratch_shapes=[
            pltpu.VMEM(tiles.shape, F32),
            pltpu.SMEM((devices,), I32),
            pltpu.SemaphoreType.DMA(()),
            pltpu.SemaphoreType.DMA(()),
        ],
        compiler_params=BIG,
        name="pack_tiles",
    )(owner, spot, tiles)


def pick_body(me, place, rows, *rest):
    outs, corner, held, sem = rest[:-3], rest[-3], rest[-2], rest[-1]
    held[...] = jnp.zeros_like(held)

    def go(i, n):
        at = place[i]

        @pl.when(at >= 0)
        def _():
            pltpu.make_async_copy(rows.at[at], held.at[i], sem).start()

        return n + (at >= 0).astype(I32)

    started = lax.fori_loop(0, place.shape[0], go, 0)

    def finish(i, carry):
        pltpu.make_async_copy(rows.at[0], held.at[0], sem).wait()
        return carry

    lax.fori_loop(0, started, finish, 0)
    for g in range(2):
        corner[:, g * LANES : (g + 1) * LANES] = held[:, g, :]
    for t, out in enumerate(outs):
        share = out.shape[0]
        out[...] = held[pl.ds(lax.rem(me[0] + t, len(outs)) * share, share)]


def pick(me, place, rows, count):
    total = place.shape[0]
    vmem = pl.BlockSpec(memory_space=pltpu.VMEM)
    return pl.pallas_call(
        pick_body,
        in_specs=[SMEM, SMEM, ANY],
        out_specs=[vmem] * (count + 1),
        out_shape=[jax.ShapeDtypeStruct((total // count, GROUPS, LANES), F32)] * count
        + [jax.ShapeDtypeStruct((total, NB), F32)],
        scratch_shapes=[pltpu.VMEM((total, GROUPS, LANES), F32), pltpu.SemaphoreType.DMA(())],
        compiler_params=BIG,
        name="pick_rows",
    )(me, place, rows)


def collect_body(*refs):
    total = refs[0][...]
    for ref in refs[1:-1]:
        total = total + ref[...]
    refs[-1][...] = total


def collect(given):
    vmem = pl.BlockSpec(memory_space=pltpu.VMEM)
    return pl.pallas_call(
        collect_body,
        in_specs=[vmem] * len(given),
        out_specs=vmem,
        out_shape=jax.ShapeDtypeStruct(given[0].shape, F32),
        compiler_params=BIG,
        name="collect_rows",
    )(*given)


def parcel_body(turn, row, rows, *rest):
    outs, seen, sem = rest[:-2], rest[-2], rest[-1]
    for t in range(len(outs)):
        seen[t] = 0

    def go(i, n):
        to = turn[i]
        at = seen[jnp.maximum(to, 0)]
        fits = (to >= 0) & (at < PARCEL)

        @pl.when(fits)
        def _():
            seen[to] = at + 1
            for t, out in enumerate(outs):

                @pl.when(to == t)
                def _():
                    pltpu.make_async_copy(rows.at[row[i]], out.at[at], sem).start()

        return n + fits.astype(I32)

    started = lax.fori_loop(0, turn.shape[0], go, 0)

    def finish(i, carry):
        pltpu.make_async_copy(rows.at[0], outs[0].at[0], sem).wait()
        return carry

    lax.fori_loop(0, started, finish, 0)


def parcel(turn, row, rows, count):
    vmem = pl.BlockSpec(memory_space=pltpu.VMEM)
    return pl.pallas_call(
        parcel_body,
        in_specs=[SMEM, SMEM, ANY],
        out_specs=[vmem] * count,
        out_shape=[jax.ShapeDtypeStruct((PARCEL, GROUPS, LANES), F32)] * count,
        scratch_shapes=[pltpu.SMEM((count,), I32), pltpu.SemaphoreType.DMA(())],
        compiler_params=BIG,
        name="parcel_rows",
    )(turn, row, rows)


def land_body(ranked, turn, row, was, rows, corner, notes, *rest):
    parcels = rest[:-8]
    out, parts, stack, seen, at_row, at_turn, at_rank, total = rest[-8:]
    step = pl.program_id(0)
    tall = rows.shape[0]
    height = tall // 2
    share = corner.shape[0] // 2

    @pl.when(step == 0)
    def _():
        for t, given in enumerate(parcels):
            seen[t] = 0
            stack[t] = given[...]

        def note(i, n):
            to = turn[i]

            @pl.when(to >= 0)
            def _():
                at_row[n] = row[i]
                at_turn[n] = to
                rank = seen[to]
                seen[to] = rank + 1
                at_rank[n] = jnp.minimum(rank, PARCEL - 1) if ranked else was[i]

            return n + (to >= 0).astype(I32)

        total[0] = lax.fori_loop(0, turn.shape[0], note, 0)

    out[...] = rows[...]
    first = step * tall

    def settle(i, carry):
        at = at_row[i] - first

        @pl.when((at >= 0) & (at < tall))
        def _():
            out[at] = stack[at_turn[i], at_rank[i]]

        return carry

    lax.fori_loop(0, total[0], settle, 0)
    for s in range(2):
        for g in range(2):
            parts[s, :height, g * LANES : (g + 1) * LANES] = out[s * height : (s + 1) * height, g, :]
        parts[s, height : height + share] = corner[s * share : (s + 1) * share]
        parts[s, height + share :] = notes[s]


def land_rows(turn, row, was, rows, corner, notes, parcels, ranked):
    count = notes.shape[0]
    tall = rows.shape[0] // count * 2
    share = corner.shape[0] // count
    slab = pl.BlockSpec((tall, GROUPS, LANES), lambda i: (i, 0, 0))
    events = turn.shape[0]
    length = tall // 2 + share + notes.shape[1]

    def body(*refs):
        return land_body(ranked, *refs)

    return pl.pallas_call(
        body,
        grid=(count // 2,),
        in_specs=[
            SMEM,
            SMEM,
            SMEM,
            slab,
            pl.BlockSpec((2 * share, NB), lambda i: (i, 0)),
            pl.BlockSpec((2,) + notes.shape[1:], lambda i: (i, 0, 0)),
        ]
        + [pl.BlockSpec(p.shape, lambda i: (0, 0, 0)) for p in parcels],
        out_specs=[slab, pl.BlockSpec((2, length, NB), lambda i: (i, 0, 0))],
        out_shape=[
            jax.ShapeDtypeStruct(rows.shape, F32),
            jax.ShapeDtypeStruct((count, length, NB), F32),
        ],
        scratch_shapes=[
            pltpu.VMEM((len(parcels),) + parcels[0].shape, F32),
            pltpu.SMEM((len(parcels),), I32),
            pltpu.SMEM((events,), I32),
            pltpu.SMEM((events,), I32),
            pltpu.SMEM((events,), I32),
            pltpu.SMEM((1,), I32),
        ],
        compiler_params=BIG,
        name="land_ranked" if ranked else "land_whole",
    )(turn, row, was, rows, corner, notes, *parcels)


def main_body(me, linv, uinv, gathered, panels, block, *rest):
    chunks = rest[:-9]
    out, chosen, final, upper, upper_hi, upper_lo, factor, corner, sem = rest[-9:]
    step = pl.program_id(0)
    height = panels.shape[2]

    def ui(k):
        return halves(uinv[k])

    @pl.when(step == 0)
    def _():
        copy = pltpu.make_async_copy(gathered.at[:, :, pl.ds(height, corner.shape[2]), :], corner, sem)
        copy.start()
        for t, chunk in enumerate(chunks):
            share = chunk.shape[0]
            chosen[pl.ds(lax.rem(me[0] - t + len(chunks), len(chunks)) * share, share)] = chunk[...]
        copy.wait()
        cols = [corner[:, k].reshape(STEPS * NB, NB) for k in range(STEPS)]
        n = [[cols[k][i * NB : (i + 1) * NB] for k in range(STEPS)] for i in range(STEPS)]
        low = {}
        for k in range(STEPS):
            x = chosen[k * NB : (k + 1) * NB].reshape(NB, GROUPS * LANES)
            for m in range(k):
                x = x - product(low[k, m], (upper_hi[m * NB : (m + 1) * NB], upper_lo[m * NB : (m + 1) * NB]))
            u = product(halves(linv[k]), halves(x))
            hi, lo = halves(u)
            upper[k * NB : (k + 1) * NB] = u
            upper_hi[k * NB : (k + 1) * NB] = hi
            upper_lo[k * NB : (k + 1) * NB] = lo
            final[k, k] = n[k][k]
            for i in range(k + 1, STEPS):
                l = product(halves(n[i][k]), ui(k))
                low[i, k] = halves(l)
                final[i, k] = l
                v = product(halves(linv[k]), halves(n[k][i]))
                final[k, i] = v
            for i in range(k + 1, STEPS):
                for j in range(k + 1, STEPS):
                    n[i][j] = n[i][j] - product(low[i, k], halves(final[k, j]))

    hi = []
    lo = []
    for k in range(STEPS):
        x = panels[:, k].reshape(2 * height, NB)
        for m in range(k):
            x = x - product((hi[m], lo[m]), halves(final[m, k]))
        l = product(halves(x), ui(k))
        factor[k] = l
        h, w = halves(l)
        hi.append(h)
        lo.append(w)
    high = jnp.concatenate(hi, axis=1)
    rest = jnp.concatenate(lo, axis=1)
    update = product((high, rest), (upper_hi[...], upper_lo[...]))
    value = block[...].reshape(2 * height, GROUPS * LANES) - update
    for s in range(2):
        for g in range(GROUPS):
            out[s, g] = value[s * height : (s + 1) * height, g * LANES : (g + 1) * LANES]

    @pl.when(me[1] < STEPS)
    def _():
        for s in range(2):
            for g in range(2):
                out[s, g] = factor[me[1], s * height : (s + 1) * height, g * LANES : (g + 1) * LANES]

    is_top = (step == 0) & (me[0] < STEPS)

    @pl.when(is_top)
    def _():
        base = me[0] * NB
        for s in range(2):
            u = upper[pl.ds(base + s * height, height), :]
            for g in range(GROUPS):
                out[s, g] = u[:, g * LANES : (g + 1) * LANES]

    @pl.when(is_top & (me[1] < STEPS))
    def _():
        for s in range(2):
            for g in range(2):
                out[s, g] = final[me[0], me[1], s * height : (s + 1) * height, g * LANES : (g + 1) * LANES]


def eliminate(me, linv, uinv, gathered, rows, chunks):
    parts, _, both, _ = gathered.shape
    height = rows.shape[0] // parts
    share = both - height
    width = GROUPS * LANES
    whole3 = pl.BlockSpec((STEPS, NB, NB), lambda i: (0, 0, 0))
    return pl.pallas_call(
        main_body,
        grid=(parts // 2,),
        in_specs=[
            SMEM,
            whole3,
            whole3,
            ANY,
            pl.BlockSpec((2, STEPS, height, NB), lambda i: (i, 0, 0, 0)),
            pl.BlockSpec((2 * height, GROUPS, LANES), lambda i: (i, 0, 0)),
        ]
        + [pl.BlockSpec(c.shape, lambda i: (0, 0, 0)) for c in chunks],
        out_specs=pl.BlockSpec((2, GROUPS, height, LANES), lambda i: (i, 0, 0, 0)),
        out_shape=jax.ShapeDtypeStruct((parts, GROUPS, height, LANES), F32),
        scratch_shapes=[
            pltpu.VMEM((STEPS * NB, GROUPS, LANES), F32),
            pltpu.VMEM((STEPS, STEPS, NB, NB), F32),
            pltpu.VMEM((STEPS * NB, width), F32),
            pltpu.VMEM((STEPS * NB, width), BF16),
            pltpu.VMEM((STEPS * NB, width), BF16),
            pltpu.VMEM((STEPS, NB, NB), F32),
            pltpu.VMEM((parts, STEPS, share, NB), F32),
            pltpu.SemaphoreType.DMA(()),
        ],
        compiler_params=BIG,
        name="eliminate",
    )(me, linv, uinv, gathered, gathered, rows, *chunks)


def tail_body(ids, base, received, out, acc, ring, staged, order, base_sem, ring_sem, out_sem):
    whole = pltpu.make_async_copy(base, acc, base_sem)
    whole.start()
    edge = acc.shape[1]

    def note(i, n):
        order[n] = i
        return n + (ids[i] >= 0).astype(I32)

    total = lax.fori_loop(0, ids.shape[0], note, 0)

    def fetch(j):
        b = lax.rem(j, RING)
        return pltpu.make_async_copy(received.at[order[j]], ring.at[b], ring_sem.at[b])

    def prime(j, carry):
        fetch(j).start()
        return carry

    lax.fori_loop(0, jnp.minimum(total, RING), prime, 0)
    whole.wait()

    def add(j, carry):
        fetch(j).wait()
        m = ids[order[j]]
        acc[m] = acc[m] + ring[lax.rem(j, RING)]

        @pl.when(j + RING < total)
        def _():
            fetch(j + RING).start()

        return carry

    lax.fori_loop(0, total, add, 0)
    copies = []
    for s in range(acc.shape[0] // GROUPS):
        p = s % 2
        if s >= 2:
            copies[s - 2].wait()
        for g in range(GROUPS):
            staged[p, :, g, :] = acc[s * GROUPS + g]
        copy = pltpu.make_async_copy(staged.at[p], out.at[pl.ds(s * edge, edge)], out_sem.at[p])
        copy.start()
        copies.append(copy)
    copies[-2].wait()
    copies[-1].wait()


def add_tiles(ids, base, received):
    spots, edge, _ = base.shape
    return pl.pallas_call(
        tail_body,
        in_specs=[SMEM, ANY, ANY],
        out_specs=ANY,
        out_shape=jax.ShapeDtypeStruct((spots // GROUPS * edge, GROUPS, LANES), F32),
        scratch_shapes=[
            pltpu.VMEM((spots, edge, LANES), F32),
            pltpu.VMEM((RING, edge, LANES), F32),
            pltpu.VMEM((2, edge, GROUPS, LANES), F32),
            pltpu.SMEM((ids.shape[0],), I32),
            pltpu.SemaphoreType.DMA(()),
            pltpu.SemaphoreType.DMA((RING,)),
            pltpu.SemaphoreType.DMA((2,)),
        ],
        compiler_params=BIG,
        name="add_tiles",
    )(ids, base, received)


def look(x, t, values, other):
    same = x[:, None] == t[None, :]
    hit = jnp.any(same, axis=1)
    return hit, jnp.where(hit, jnp.sum(jnp.where(same, values[None, :], 0), axis=1), other)


def permutation(swap_rows):
    t0, t1, t2 = swap_rows[0], swap_rows[1], swap_rows[2]
    j = jnp.arange(NB, dtype=I32)
    n = NB
    x = jnp.concatenate([NB + j, 2 * NB + j, t1, t2])
    _, once = look(x, t0, j, x)
    v1 = once[:n]
    y = jnp.concatenate([2 * NB + j, t2])
    _, twice = look(y, t1, v1, jnp.concatenate([once[n : 2 * n], once[3 * n :]]))
    v2 = twice[:n]
    source = jnp.concatenate([t0, once[2 * n : 3 * n], twice[n:]])
    below = STEPS * NB
    in1 = jnp.any(t0[:, None] == t1[None, :], axis=1)
    in2 = jnp.any(jnp.concatenate([t0, t1])[:, None] == t2[None, :], axis=1)
    ok0 = (t0 >= below) & ~in1 & ~in2[:n]
    ok1 = (t1 >= below) & ~in2[n:]
    ok2 = t2 >= below
    land = jnp.where(jnp.concatenate([ok0, ok1, ok2]), jnp.concatenate([t0, t1, t2]), -1)
    return source, land, jnp.concatenate([j, v1, v2])


def step(front_matrix, swap_rows, l_inverse, u_inverse, contrib_tiles, tile_owner, tile_spot):
    row_count = lax.axis_size("row")
    col_count = lax.axis_size("col")
    row_place = lax.axis_index("row").astype(I32)
    col_place = lax.axis_index("col").astype(I32)
    me = jnp.stack([row_place, col_place])
    local_rows = front_matrix.shape[0] * NB
    rows = front_matrix.reshape(-1).reshape(local_rows, GROUPS, LANES)

    def exchange(x, axes):
        return lax.all_to_all(x, axes, split_axis=0, concat_axis=0, tiled=True)

    def shift(x, t):
        return lax.ppermute(x, "row", [(p, (p + t) % row_count) for p in range(row_count)])

    def leave(x, t):
        return lax.ppermute(x, "row", [(p, (p + t) % row_count) for p in range(STEPS)])

    def home(x):
        block = x // NB
        here = (x >= 0) & (block % row_count == row_place)
        return jnp.where(here, block // row_count * NB + x % NB, -1)

    source, land, old = permutation(swap_rows)
    from_row = old // NB
    to_row = land // NB % row_count
    going = jnp.where((land >= 0) & (from_row == row_place), (to_row - row_place) % row_count, -1)
    coming = jnp.where((land >= 0) & (to_row == row_place), (row_place - from_row) % row_count, -1)
    pair = jnp.where(land >= 0, from_row * row_count + to_row, -1)
    loads = jnp.sum((pair[:, None] == jnp.arange(STEPS * row_count, dtype=I32)[None, :]).astype(I32), axis=0)

    parcels = parcel(going, old % NB, rows, row_count)
    parcels = [parcels[0]] + [leave(parcels[t], t) for t in range(1, row_count)]
    picked = pick(me, home(source), rows, row_count)
    picked, corner = list(picked[:-1]), picked[-1]
    given = [picked[0]] + [shift(picked[t], t) for t in range(1, row_count)]
    send, ids = pack(contrib_tiles, tile_owner[:, 0], tile_spot, row_count * col_count)
    notes = ids.astype(F32).reshape(row_count, col_count, CAP).transpose(1, 0, 2).reshape(col_count, -1)
    notes = jnp.pad(notes[:, None, :], ((0, 0), (0, 7), (0, NB - notes.shape[1])))

    def ranked(parcels):
        return land_rows(coming, home(land), old % NB, rows, corner, notes, parcels, True)

    def whole(parcels):
        every = [rows[:NB]] + [leave(rows[:NB], t) for t in range(1, row_count)]
        return land_rows(coming, home(land), old % NB, rows, corner, notes, every, False)

    moved, parts = lax.cond(jnp.max(loads) > PARCEL, whole, ranked, parcels)
    dealt = exchange(parts, "col")
    tall = local_rows // col_count
    partial = dealt[:STEPS, tall:-8].reshape(-1, NB)
    notes = dealt[:, -8, : row_count * CAP].reshape(col_count, row_count, CAP).transpose(1, 0, 2)
    notes = jnp.pad(notes.reshape(1, -1), ((0, 7), (0, NB - notes.size)))
    partial = jnp.concatenate([partial, notes])
    partial = jnp.stack([partial] + [shift(partial, t) for t in range(1, row_count)])
    corner = jnp.sum(partial[:, :-8], axis=0).reshape(STEPS, -1, NB)
    mixed = jnp.concatenate([dealt[:STEPS, :tall], corner], axis=1)
    gathered = lax.all_gather(mixed.reshape(-1, NB), "col", axis=0, tiled=True)
    gathered = gathered.reshape(col_count, STEPS, -1, NB)
    notes = partial[:, -8].reshape(row_count, -1)[:, : row_count * col_count * CAP]
    notes = lax.dynamic_slice_in_dim(notes, row_place * col_count * CAP, col_count * CAP, 1)
    turn = (row_place - jnp.arange(row_count, dtype=I32)) % row_count
    ids_in = notes[turn].reshape(-1).astype(I32)
    summed = collect(given)
    chunks = [summed] + [shift(summed, t) for t in range(1, row_count)]
    send, gathered, *chunks = lax.optimization_barrier((send, gathered, *chunks))
    received = exchange(send, ("row", "col"))
    base = eliminate(me, l_inverse, u_inverse, gathered, moved, chunks)
    out = add_tiles(ids_in, base.reshape(-1, LANES, LANES), received)
    return out.reshape(-1).reshape(front_matrix.shape)


def solution(mesh):
    placed = (
        P(None, "row", None, None, "col", None),
        P(),
        P(),
        P(),
        P(("row", "col"), None, None),
        P(("row", "col"), None),
        P(("row", "col")),
    )
    return jax.shard_map(
        step,
        mesh=mesh,
        in_specs=placed,
        out_specs=P(None, "row", None, None, "col", None),
        check_vma=False,
    )
```

```python
import jax
import jax.numpy as jnp
from jax import lax
from jax.experimental import pallas as pl
from jax.experimental.pallas import tpu as pltpu
from jax.sharding import PartitionSpec as P


STEPS = 3
CAP = 2
NB = 256
LANES = 128
GROUPS = 8
RING = 16
PARCEL = 48
F32 = jnp.float32
BF16 = jnp.bfloat16
I32 = jnp.int32
ANY = pl.BlockSpec(memory_space=pl.ANY)
SMEM = pl.BlockSpec(memory_space=pltpu.SMEM)


def room(mib):
    return pltpu.CompilerParams(vmem_limit_bytes=mib * 1024 * 1024)


def halves(x):
    high = x.astype(BF16)
    return high, (x - high.astype(F32)).astype(BF16)


def product(a, b):
    def one(x, y):
        return jnp.dot(x, y, preferred_element_type=F32)

    return one(a[0], b[0]) + (one(a[0], b[1]) + one(a[1], b[0]))


def pack_body(owner, spot, tiles, *rest):
    send, ids, held, seen, load_sem, sem = rest[-6:]
    count = tiles.shape[0]
    load = pltpu.make_async_copy(tiles, held, load_sem)
    load.start()

    def clear(i, carry):
        ids[i] = -1
        return carry

    def fresh(i, carry):
        seen[i] = 0
        return carry

    lax.fori_loop(0, ids.shape[0], clear, 0)
    lax.fori_loop(0, seen.shape[0], fresh, 0)
    load.wait()

    def put(i, carry):
        d = owner[i]
        rank = seen[d]
        seen[d] = rank + 1
        slot = d * CAP + rank
        ids[slot] = spot[i]
        pltpu.make_async_copy(held.at[i], send.at[slot], sem).start()
        return carry

    lax.fori_loop(0, count, put, 0)
    pltpu.make_async_copy(held, send.at[pl.ds(0, count)], sem).wait()


def pack(tiles, owner, spot, devices):
    edge = tiles.shape[1]
    return pl.pallas_call(
        pack_body,
        in_specs=[SMEM, SMEM, ANY],
        out_specs=[ANY, SMEM],
        out_shape=[
            jax.ShapeDtypeStruct((devices * CAP, edge, edge), F32),
            jax.ShapeDtypeStruct((devices * CAP,), I32),
        ],
        scratch_shapes=[
            pltpu.VMEM(tiles.shape, F32),
            pltpu.SMEM((devices,), I32),
            pltpu.SemaphoreType.DMA(()),
            pltpu.SemaphoreType.DMA(()),
        ],
        compiler_params=room(10),
        name="pack_tiles",
    )(owner, spot, tiles)


def pick_body(me, leaving, place, rows, *rest):
    count = (len(rest) - 4) // 2
    parcels, outs = rest[:count], rest[count : 2 * count]
    corner, held, sem, leave_sem = rest[2 * count :]
    cap = parcels[0].shape[0]
    share = outs[0].shape[0]
    sent = jnp.int32(0)
    for t in range(count):

        def fill(i, n, t=t):
            at = leaving[t * cap + i]

            @pl.when(at >= 0)
            def _():
                pltpu.make_async_copy(rows.at[at], parcels[t].at[i], leave_sem).start()

            return n + (at >= 0).astype(I32)

        sent = lax.fori_loop(0, cap, fill, sent)
    held[...] = jnp.zeros_like(held)

    def go(i, n):
        at = place[i]

        @pl.when(at >= 0)
        def _():
            pltpu.make_async_copy(rows.at[at], held.at[i], sem).start()

        return n + (at >= 0).astype(I32)

    started = lax.fori_loop(0, place.shape[0], go, 0)

    def finish(i, carry):
        pltpu.make_async_copy(rows.at[0], held.at[0], sem).wait()
        return carry

    def finish_leave(i, carry):
        pltpu.make_async_copy(rows.at[0], parcels[0].at[0], leave_sem).wait()
        return carry

    lax.fori_loop(0, sent, finish_leave, 0)
    lax.fori_loop(0, started, finish, 0)
    for g in range(2):
        corner[:, g * LANES : (g + 1) * LANES] = held[:, g, :]
    for t, out in enumerate(outs):
        out[...] = held[pl.ds(lax.rem(me[0] + t, count) * share, share)]


def pick(me, leaving, place, rows, count):
    total = place.shape[0]
    cap = leaving.shape[0] // count
    vmem = pl.BlockSpec(memory_space=pltpu.VMEM)
    return pl.pallas_call(
        pick_body,
        in_specs=[SMEM, SMEM, SMEM, ANY],
        out_specs=[vmem] * (2 * count + 1),
        out_shape=[jax.ShapeDtypeStruct((cap, GROUPS, LANES), F32)] * count
        + [jax.ShapeDtypeStruct((total // count, GROUPS, LANES), F32)] * count
        + [jax.ShapeDtypeStruct((total, NB), F32)],
        scratch_shapes=[
            pltpu.VMEM((total, GROUPS, LANES), F32),
            pltpu.SemaphoreType.DMA(()),
            pltpu.SemaphoreType.DMA(()),
        ],
        compiler_params=room(16),
        name="pick_rows",
    )(me, leaving, place, rows)


def collect_body(*refs):
    total = refs[0][...]
    for ref in refs[1:-1]:
        total = total + ref[...]
    refs[-1][...] = total


def collect(given):
    vmem = pl.BlockSpec(memory_space=pltpu.VMEM)
    return pl.pallas_call(
        collect_body,
        in_specs=[vmem] * len(given),
        out_specs=vmem,
        out_shape=jax.ShapeDtypeStruct(given[0].shape, F32),
        compiler_params=room(10),
        name="collect_rows",
    )(*given)


def land_body(landing, rows, corner, notes, *rest):
    parcels = rest[:-5]
    out, parts, held, sem, out_sem = rest[-5:]
    load = pltpu.make_async_copy(rows, held, sem)
    load.start()
    share = corner.shape[0] // parts.shape[0]
    height = held.shape[0] // parts.shape[0]

    def head(s, carry):
        parts[s, height : height + share] = corner[pl.ds(pl.multiple_of(s * share, 8), share)]
        parts[s, height + share :] = notes[s]
        return carry

    lax.fori_loop(0, parts.shape[0], head, 0)
    load.wait()
    for t, given in enumerate(parcels):
        cap = given.shape[0]

        def settle(i, carry, t=t, given=given, cap=cap):
            at = landing[t * cap + i]

            @pl.when(at >= 0)
            def _():
                held[at] = given[i]

            return carry

        lax.fori_loop(0, cap, settle, 0)
    save = pltpu.make_async_copy(held, out, out_sem)
    save.start()

    def body(s, carry):
        for g in range(2):
            parts[s, :height, g * LANES : (g + 1) * LANES] = held[pl.ds(s * height, height), g, :]
        return carry

    lax.fori_loop(0, parts.shape[0], body, 0)
    save.wait()


def land_rows(landing, rows, corner, notes, parcels):
    count = notes.shape[0]
    vmem = pl.BlockSpec(memory_space=pltpu.VMEM)
    length = rows.shape[0] // count + corner.shape[0] // count + notes.shape[1]
    return pl.pallas_call(
        land_body,
        in_specs=[SMEM, ANY, vmem, vmem] + [vmem] * len(parcels),
        out_specs=[ANY, vmem],
        out_shape=[
            jax.ShapeDtypeStruct(rows.shape, F32),
            jax.ShapeDtypeStruct((count, length, NB), F32),
        ],
        scratch_shapes=[
            pltpu.VMEM(rows.shape, F32),
            pltpu.SemaphoreType.DMA(()),
            pltpu.SemaphoreType.DMA(()),
        ],
        compiler_params=room(28),
    )(landing, rows, corner, notes, *parcels)


def main_body(me, linv, uinv, gathered, panels, block, *rest):
    chunks = rest[:-9]
    out, chosen, final, upper, upper_hi, upper_lo, factor, corner, sem = rest[-9:]
    step = pl.program_id(0)
    height = panels.shape[2]

    def ui(k):
        return halves(uinv[k])

    @pl.when(step == 0)
    def _():
        copy = pltpu.make_async_copy(gathered.at[:, :, pl.ds(height, corner.shape[2]), :], corner, sem)
        copy.start()
        for t, chunk in enumerate(chunks):
            share = chunk.shape[0]
            chosen[pl.ds(lax.rem(me[0] - t + len(chunks), len(chunks)) * share, share)] = chunk[...]
        copy.wait()
        cols = [corner[:, k].reshape(STEPS * NB, NB) for k in range(STEPS)]
        n = [[cols[k][i * NB : (i + 1) * NB] for k in range(STEPS)] for i in range(STEPS)]
        low = {}
        for k in range(STEPS):
            x = chosen[k * NB : (k + 1) * NB].reshape(NB, GROUPS * LANES)
            for m in range(k):
                x = x - product(low[k, m], (upper_hi[m * NB : (m + 1) * NB], upper_lo[m * NB : (m + 1) * NB]))
            u = product(halves(linv[k]), halves(x))
            hi, lo = halves(u)
            upper[k * NB : (k + 1) * NB] = u
            upper_hi[k * NB : (k + 1) * NB] = hi
            upper_lo[k * NB : (k + 1) * NB] = lo
            final[k, k] = n[k][k]
            for i in range(k + 1, STEPS):
                l = product(halves(n[i][k]), ui(k))
                low[i, k] = halves(l)
                final[i, k] = l
                v = product(halves(linv[k]), halves(n[k][i]))
                final[k, i] = v
            for i in range(k + 1, STEPS):
                for j in range(k + 1, STEPS):
                    n[i][j] = n[i][j] - product(low[i, k], halves(final[k, j]))

    hi = []
    lo = []
    for k in range(STEPS):
        x = panels[:, k].reshape(2 * height, NB)
        for m in range(k):
            x = x - product((hi[m], lo[m]), halves(final[m, k]))
        l = product(halves(x), ui(k))
        factor[k] = l
        h, w = halves(l)
        hi.append(h)
        lo.append(w)
    high = jnp.concatenate(hi, axis=1)
    rest = jnp.concatenate(lo, axis=1)
    update = product((high, rest), (upper_hi[...], upper_lo[...]))
    value = block[...].reshape(2 * height, GROUPS * LANES) - update
    for s in range(2):
        for g in range(GROUPS):
            out[s, g] = value[s * height : (s + 1) * height, g * LANES : (g + 1) * LANES]

    @pl.when(me[1] < STEPS)
    def _():
        for s in range(2):
            for g in range(2):
                out[s, g] = factor[me[1], s * height : (s + 1) * height, g * LANES : (g + 1) * LANES]

    is_top = (step == 0) & (me[0] < STEPS)

    @pl.when(is_top)
    def _():
        base = me[0] * NB
        for s in range(2):
            u = upper[pl.ds(base + s * height, height), :]
            for g in range(GROUPS):
                out[s, g] = u[:, g * LANES : (g + 1) * LANES]

    @pl.when(is_top & (me[1] < STEPS))
    def _():
        for s in range(2):
            for g in range(2):
                out[s, g] = final[me[0], me[1], s * height : (s + 1) * height, g * LANES : (g + 1) * LANES]


def eliminate(me, linv, uinv, gathered, rows, chunks):
    parts, _, both, _ = gathered.shape
    height = rows.shape[0] // parts
    share = both - height
    width = GROUPS * LANES
    whole3 = pl.BlockSpec((STEPS, NB, NB), lambda i: (0, 0, 0))
    return pl.pallas_call(
        main_body,
        grid=(parts // 2,),
        in_specs=[
            SMEM,
            whole3,
            whole3,
            ANY,
            pl.BlockSpec((2, STEPS, height, NB), lambda i: (i, 0, 0, 0)),
            pl.BlockSpec((2 * height, GROUPS, LANES), lambda i: (i, 0, 0)),
        ]
        + [pl.BlockSpec(c.shape, lambda i: (0, 0, 0)) for c in chunks],
        out_specs=pl.BlockSpec((2, GROUPS, height, LANES), lambda i: (i, 0, 0, 0)),
        out_shape=jax.ShapeDtypeStruct((parts, GROUPS, height, LANES), F32),
        scratch_shapes=[
            pltpu.VMEM((STEPS * NB, GROUPS, LANES), F32),
            pltpu.VMEM((STEPS, STEPS, NB, NB), F32),
            pltpu.VMEM((STEPS * NB, width), F32),
            pltpu.VMEM((STEPS * NB, width), BF16),
            pltpu.VMEM((STEPS * NB, width), BF16),
            pltpu.VMEM((STEPS, NB, NB), F32),
            pltpu.VMEM((parts, STEPS, share, NB), F32),
            pltpu.SemaphoreType.DMA(()),
        ],
        compiler_params=room(42),
        name="eliminate",
    )(me, linv, uinv, gathered, gathered, rows, *chunks)


def tail_body(ids, base, received, out, acc, ring, staged, order, base_sem, ring_sem, out_sem):
    whole = pltpu.make_async_copy(base, acc, base_sem)
    whole.start()
    edge = acc.shape[1]

    def note(i, n):
        order[n] = i
        return n + (ids[i] >= 0).astype(I32)

    total = lax.fori_loop(0, ids.shape[0], note, 0)

    def fetch(j):
        b = lax.rem(j, RING)
        return pltpu.make_async_copy(received.at[order[j]], ring.at[b], ring_sem.at[b])

    def prime(j, carry):
        fetch(j).start()
        return carry

    lax.fori_loop(0, jnp.minimum(total, RING), prime, 0)
    whole.wait()

    def add(j, carry):
        fetch(j).wait()
        m = ids[order[j]]
        acc[m] = acc[m] + ring[lax.rem(j, RING)]

        @pl.when(j + RING < total)
        def _():
            fetch(j + RING).start()

        return carry

    lax.fori_loop(0, total, add, 0)
    strips = acc.shape[0] // GROUPS

    def writing(s):
        p = lax.rem(s, 2)
        return pltpu.make_async_copy(staged.at[p], out.at[pl.ds(s * edge, edge)], out_sem.at[p])

    def strip(s, carry):
        p = lax.rem(s, 2)

        @pl.when(s >= 2)
        def _():
            writing(s - 2).wait()

        for g in range(GROUPS):
            staged[p, :, g, :] = acc[s * GROUPS + g]
        writing(s).start()
        return carry

    lax.fori_loop(0, strips, strip, 0)
    writing(jnp.int32(strips - 2)).wait()
    writing(jnp.int32(strips - 1)).wait()


def add_tiles(ids, base, received):
    spots, edge, _ = base.shape
    return pl.pallas_call(
        tail_body,
        in_specs=[SMEM, ANY, ANY],
        out_specs=ANY,
        out_shape=jax.ShapeDtypeStruct((spots // GROUPS * edge, GROUPS, LANES), F32),
        scratch_shapes=[
            pltpu.VMEM((spots, edge, LANES), F32),
            pltpu.VMEM((RING, edge, LANES), F32),
            pltpu.VMEM((2, edge, GROUPS, LANES), F32),
            pltpu.SMEM((ids.shape[0],), I32),
            pltpu.SemaphoreType.DMA(()),
            pltpu.SemaphoreType.DMA((RING,)),
            pltpu.SemaphoreType.DMA((2,)),
        ],
        compiler_params=room(14),
        name="add_tiles",
    )(ids, base, received)


def look(x, t, values, other):
    same = x[:, None] == t[None, :]
    hit = jnp.any(same, axis=1)
    return hit, jnp.where(hit, jnp.sum(jnp.where(same, values[None, :], 0), axis=1), other)


def permutation(swap_rows):
    t0, t1, t2 = swap_rows[0], swap_rows[1], swap_rows[2]
    j = jnp.arange(NB, dtype=I32)
    n = NB
    x = jnp.concatenate([NB + j, 2 * NB + j, t1, t2])
    _, once = look(x, t0, j, x)
    v1 = once[:n]
    y = jnp.concatenate([2 * NB + j, t2])
    _, twice = look(y, t1, v1, jnp.concatenate([once[n : 2 * n], once[3 * n :]]))
    v2 = twice[:n]
    source = jnp.concatenate([t0, once[2 * n : 3 * n], twice[n:]])
    below = STEPS * NB
    in1 = jnp.any(t0[:, None] == t1[None, :], axis=1)
    in2 = jnp.any(jnp.concatenate([t0, t1])[:, None] == t2[None, :], axis=1)
    ok0 = (t0 >= below) & ~in1 & ~in2[:n]
    ok1 = (t1 >= below) & ~in2[n:]
    ok2 = t2 >= below
    land = jnp.where(jnp.concatenate([ok0, ok1, ok2]), jnp.concatenate([t0, t1, t2]), -1)
    return source, land, jnp.concatenate([j, v1, v2])


def ranks(turn):
    i = jnp.arange(turn.shape[0], dtype=I32)
    earlier = (turn[:, None] == turn[None, :]) & (i[None, :] < i[:, None])
    return jnp.sum(earlier.astype(I32), axis=1)


def slots(turn, rank, cap, count, value):
    slot = jnp.where((turn >= 0) & (rank < cap), turn * cap + rank, -1)
    place = jnp.arange(count * cap, dtype=I32)
    same = slot[None, :] == place[:, None]
    return jnp.sum(jnp.where(same, value[None, :] + 1, 0), axis=1) - 1


def step(front_matrix, swap_rows, l_inverse, u_inverse, contrib_tiles, tile_owner, tile_spot):
    row_count = lax.axis_size("row")
    col_count = lax.axis_size("col")
    row_place = lax.axis_index("row").astype(I32)
    col_place = lax.axis_index("col").astype(I32)
    me = jnp.stack([row_place, col_place])
    local_rows = front_matrix.shape[0] * NB
    rows = front_matrix.reshape(-1).reshape(local_rows, GROUPS, LANES)

    def exchange(x, axes):
        return lax.all_to_all(x, axes, split_axis=0, concat_axis=0, tiled=True)

    def shift(x, t):
        return lax.ppermute(x, "row", [(p, (p + t) % row_count) for p in range(row_count)])

    def leave(x, t):
        return lax.ppermute(x, "row", [(p, (p + t) % row_count) for p in range(STEPS)])

    def home(x):
        block = x // NB
        here = (x >= 0) & (block % row_count == row_place)
        return jnp.where(here, block // row_count * NB + x % NB, -1)

    source, land, old = permutation(swap_rows)
    from_row = old // NB
    to_row = land // NB % row_count
    going = jnp.where((land >= 0) & (from_row == row_place), (to_row - row_place) % row_count, -1)
    coming = jnp.where((land >= 0) & (to_row == row_place), (row_place - from_row) % row_count, -1)
    pair = jnp.where(land >= 0, from_row * row_count + to_row, -1)
    loads = jnp.sum((pair[:, None] == jnp.arange(STEPS * row_count, dtype=I32)[None, :]).astype(I32), axis=0)

    leaving = slots(going, ranks(going), PARCEL, row_count, old % NB)
    landing = slots(coming, ranks(coming), PARCEL, row_count, home(land))
    picked = pick(me, leaving, home(source), rows, row_count)
    parcels, picked, corner = picked[:row_count], picked[row_count:-1], picked[-1]
    parcels = [parcels[0]] + [leave(parcels[t], t) for t in range(1, row_count)]
    given = [picked[0]] + [shift(picked[t], t) for t in range(1, row_count)]
    send, ids = pack(contrib_tiles, tile_owner[:, 0], tile_spot, row_count * col_count)
    notes = ids.astype(F32).reshape(row_count, col_count, CAP).transpose(1, 0, 2).reshape(col_count, -1)
    notes = jnp.pad(notes[:, None, :], ((0, 0), (0, 7), (0, NB - notes.shape[1])))

    def ranked(parcels):
        return land_rows(landing, rows, corner, notes, parcels)

    def whole(parcels):
        every = [rows[:NB]] + [leave(rows[:NB], t) for t in range(1, row_count)]
        spread = slots(coming, old % NB, NB, row_count, home(land))
        return land_rows(spread, rows, corner, notes, every)

    moved, parts = lax.cond(jnp.max(loads) > PARCEL, whole, ranked, parcels)
    dealt = exchange(parts, "col")
    tall = local_rows // col_count
    partial = dealt[:STEPS, tall:-8].reshape(-1, NB)
    notes = dealt[:, -8, : row_count * CAP].reshape(col_count, row_count, CAP).transpose(1, 0, 2)
    notes = jnp.pad(notes.reshape(1, -1), ((0, 7), (0, NB - notes.size)))
    partial = jnp.concatenate([partial, notes])
    partial = jnp.stack([partial] + [shift(partial, t) for t in range(1, row_count)])
    corner = jnp.sum(partial[:, :-8], axis=0).reshape(STEPS, -1, NB)
    mixed = jnp.concatenate([dealt[:STEPS, :tall], corner], axis=1)
    gathered = lax.all_gather(mixed.reshape(-1, NB), "col", axis=0, tiled=True)
    gathered = gathered.reshape(col_count, STEPS, -1, NB)
    notes = partial[:, -8].reshape(row_count, -1)[:, : row_count * col_count * CAP]
    notes = lax.dynamic_slice_in_dim(notes, row_place * col_count * CAP, col_count * CAP, 1)
    turn = (row_place - jnp.arange(row_count, dtype=I32)) % row_count
    ids_in = notes[turn].reshape(-1).astype(I32)
    summed = collect(given)
    chunks = [summed] + [shift(summed, t) for t in range(1, row_count)]
    send, gathered, *chunks = lax.optimization_barrier((send, gathered, *chunks))
    received = exchange(send, ("row", "col"))
    base = eliminate(me, l_inverse, u_inverse, gathered, moved, chunks)
    out = add_tiles(ids_in, base.reshape(-1, LANES, LANES), received)
    return out.reshape(-1).reshape(front_matrix.shape)


def solution(mesh):
    placed = (
        P(None, "row", None, None, "col", None),
        P(),
        P(),
        P(),
        P(("row", "col"), None, None),
        P(("row", "col"), None),
        P(("row", "col")),
    )
    return jax.shard_map(
        step,
        mesh=mesh,
        in_specs=placed,
        out_specs=P(None, "row", None, None, "col", None),
        check_vma=False,
    )
```

```python
import jax
import jax.numpy as jnp
from jax import lax
from jax.experimental import pallas as pl
from jax.experimental.pallas import tpu as pltpu
from jax.sharding import PartitionSpec as P


STEPS = 3
CAP = 2
NB = 256
LANES = 128
GROUPS = 8
RING = 16
PARCEL = 48
F32 = jnp.float32
BF16 = jnp.bfloat16
I32 = jnp.int32
ANY = pl.BlockSpec(memory_space=pl.ANY)
SMEM = pl.BlockSpec(memory_space=pltpu.SMEM)


def room(mib):
    return pltpu.CompilerParams(vmem_limit_bytes=mib * 1024 * 1024)


def halves(x):
    high = x.astype(BF16)
    return high, (x - high.astype(F32)).astype(BF16)


def product(a, b):
    def one(x, y):
        return jnp.dot(x, y, preferred_element_type=F32)

    return one(a[0], b[0]) + (one(a[0], b[1]) + one(a[1], b[0]))


def pack_body(slot, tiles, send, held, load_sem, sem):
    count = tiles.shape[0]
    load = pltpu.make_async_copy(tiles, held, load_sem)
    load.start()
    load.wait()

    def put(i, carry):
        pltpu.make_async_copy(held.at[i], send.at[slot[i]], sem).start()
        return carry

    lax.fori_loop(0, count, put, 0)
    pltpu.make_async_copy(held, send.at[pl.ds(0, count)], sem).wait()


def pack(tiles, slot, total):
    edge = tiles.shape[1]
    return pl.pallas_call(
        pack_body,
        in_specs=[SMEM, ANY],
        out_specs=ANY,
        out_shape=jax.ShapeDtypeStruct((total, edge, edge), F32),
        scratch_shapes=[
            pltpu.VMEM(tiles.shape, F32),
            pltpu.SemaphoreType.DMA(()),
            pltpu.SemaphoreType.DMA(()),
        ],
        compiler_params=room(10),
        name="pack_tiles",
    )(slot, tiles)


def pick_body(me, leaving, place, rows, *rest):
    count = (len(rest) - 4) // 2
    parcels, outs = rest[:count], rest[count : 2 * count]
    corner, held, sem, leave_sem = rest[2 * count :]
    cap = parcels[0].shape[0]
    share = outs[0].shape[0]
    sent = jnp.int32(0)
    for t in range(count):

        def fill(i, n, t=t):
            at = leaving[t * cap + i]

            @pl.when(at >= 0)
            def _():
                pltpu.make_async_copy(rows.at[at], parcels[t].at[i], leave_sem).start()

            return n + (at >= 0).astype(I32)

        sent = lax.fori_loop(0, cap, fill, sent)
    held[...] = jnp.zeros_like(held)

    def go(i, n):
        at = place[i]

        @pl.when(at >= 0)
        def _():
            pltpu.make_async_copy(rows.at[at], held.at[i], sem).start()

        return n + (at >= 0).astype(I32)

    started = lax.fori_loop(0, place.shape[0], go, 0)

    def finish(i, carry):
        pltpu.make_async_copy(rows.at[0], held.at[0], sem).wait()
        return carry

    def finish_leave(i, carry):
        pltpu.make_async_copy(rows.at[0], parcels[0].at[0], leave_sem).wait()
        return carry

    lax.fori_loop(0, sent, finish_leave, 0)
    lax.fori_loop(0, started, finish, 0)
    for g in range(2):
        corner[:, g * LANES : (g + 1) * LANES] = held[:, g, :]
    for t, out in enumerate(outs):
        out[...] = held[pl.ds(lax.rem(me[0] + t, count) * share, share)]


def pick(me, leaving, place, rows, count):
    total = place.shape[0]
    cap = leaving.shape[0] // count
    vmem = pl.BlockSpec(memory_space=pltpu.VMEM)
    return pl.pallas_call(
        pick_body,
        in_specs=[SMEM, SMEM, SMEM, ANY],
        out_specs=[vmem] * (2 * count + 1),
        out_shape=[jax.ShapeDtypeStruct((cap, GROUPS, LANES), F32)] * count
        + [jax.ShapeDtypeStruct((total // count, GROUPS, LANES), F32)] * count
        + [jax.ShapeDtypeStruct((total, NB), F32)],
        scratch_shapes=[
            pltpu.VMEM((total, GROUPS, LANES), F32),
            pltpu.SemaphoreType.DMA(()),
            pltpu.SemaphoreType.DMA(()),
        ],
        compiler_params=room(16),
        name="pick_rows",
    )(me, leaving, place, rows)


def collect_body(*refs):
    total = refs[0][...]
    for ref in refs[1:-1]:
        total = total + ref[...]
    refs[-1][...] = total


def collect(given):
    vmem = pl.BlockSpec(memory_space=pltpu.VMEM)
    return pl.pallas_call(
        collect_body,
        in_specs=[vmem] * len(given),
        out_specs=vmem,
        out_shape=jax.ShapeDtypeStruct(given[0].shape, F32),
        compiler_params=room(10),
        name="collect_rows",
    )(*given)


def land_body(landing, rows, corner, notes, *rest):
    parcels = rest[:-5]
    out, parts, held, sem, out_sem = rest[-5:]
    load = pltpu.make_async_copy(rows, held, sem)
    load.start()
    share = corner.shape[0] // parts.shape[0]
    height = held.shape[0] // parts.shape[0]

    def head(s, carry):
        parts[s, height : height + share] = corner[pl.ds(pl.multiple_of(s * share, 8), share)]
        parts[s, height + share :] = notes[s]
        return carry

    lax.fori_loop(0, parts.shape[0], head, 0)
    load.wait()
    for t, given in enumerate(parcels):
        cap = given.shape[0]

        def settle(i, carry, t=t, given=given, cap=cap):
            at = landing[t * cap + i]

            @pl.when(at >= 0)
            def _():
                held[at] = given[i]

            return carry

        lax.fori_loop(0, cap, settle, 0)
    save = pltpu.make_async_copy(held, out, out_sem)
    save.start()

    def body(s, carry):
        for g in range(2):
            parts[s, :height, g * LANES : (g + 1) * LANES] = held[pl.ds(s * height, height), g, :]
        return carry

    lax.fori_loop(0, parts.shape[0], body, 0)
    save.wait()


def land_rows(landing, rows, corner, notes, parcels):
    count = notes.shape[0]
    vmem = pl.BlockSpec(memory_space=pltpu.VMEM)
    length = rows.shape[0] // count + corner.shape[0] // count + notes.shape[1]
    return pl.pallas_call(
        land_body,
        in_specs=[SMEM, ANY, vmem, vmem] + [vmem] * len(parcels),
        out_specs=[ANY, vmem],
        out_shape=[
            jax.ShapeDtypeStruct(rows.shape, F32),
            jax.ShapeDtypeStruct((count, length, NB), F32),
        ],
        scratch_shapes=[
            pltpu.VMEM(rows.shape, F32),
            pltpu.SemaphoreType.DMA(()),
            pltpu.SemaphoreType.DMA(()),
        ],
        compiler_params=room(28),
    )(landing, rows, corner, notes, *parcels)


def main_body(me, linv, uinv, gathered, panels, block, tiles, *rest):
    chunks = rest[:-10]
    done, out, chosen, final, upper, upper_hi, upper_lo, factor, corner, sem = rest[-10:]
    step = pl.program_id(0)
    height = panels.shape[2]

    def ui(k):
        return halves(uinv[k])

    @pl.when(step == 0)
    def _():
        copy = pltpu.make_async_copy(gathered.at[:, :, pl.ds(height, corner.shape[2]), :], corner, sem)
        copy.start()
        for t, chunk in enumerate(chunks):
            share = chunk.shape[0]
            chosen[pl.ds(lax.rem(me[0] - t + len(chunks), len(chunks)) * share, share)] = chunk[...]
        copy.wait()
        cols = [corner[:, k].reshape(STEPS * NB, NB) for k in range(STEPS)]
        n = [[cols[k][i * NB : (i + 1) * NB] for k in range(STEPS)] for i in range(STEPS)]
        low = {}
        for k in range(STEPS):
            x = chosen[k * NB : (k + 1) * NB].reshape(NB, GROUPS * LANES)
            for m in range(k):
                x = x - product(low[k, m], (upper_hi[m * NB : (m + 1) * NB], upper_lo[m * NB : (m + 1) * NB]))
            u = product(halves(linv[k]), halves(x))
            hi, lo = halves(u)
            upper[k * NB : (k + 1) * NB] = u
            upper_hi[k * NB : (k + 1) * NB] = hi
            upper_lo[k * NB : (k + 1) * NB] = lo
            final[k, k] = n[k][k]
            for i in range(k + 1, STEPS):
                l = product(halves(n[i][k]), ui(k))
                low[i, k] = halves(l)
                final[i, k] = l
                v = product(halves(linv[k]), halves(n[k][i]))
                final[k, i] = v
            for i in range(k + 1, STEPS):
                for j in range(k + 1, STEPS):
                    n[i][j] = n[i][j] - product(low[i, k], halves(final[k, j]))

    hi = []
    lo = []
    for k in range(STEPS):
        x = panels[:, k].reshape(2 * height, NB)
        for m in range(k):
            x = x - product((hi[m], lo[m]), halves(final[m, k]))
        l = product(halves(x), ui(k))
        factor[k] = l
        h, w = halves(l)
        hi.append(h)
        lo.append(w)
    high = jnp.concatenate(hi, axis=1)
    rest = jnp.concatenate(lo, axis=1)
    update = product((high, rest), (upper_hi[...], upper_lo[...]))
    value = block[...].reshape(2 * height, GROUPS * LANES) - update
    for s in range(2):
        for g in range(GROUPS):
            out[s, g] = value[s * height : (s + 1) * height, g * LANES : (g + 1) * LANES]

    @pl.when(me[1] < STEPS)
    def _():
        for s in range(2):
            for g in range(2):
                out[s, g] = factor[me[1], s * height : (s + 1) * height, g * LANES : (g + 1) * LANES]

    is_top = (step == 0) & (me[0] < STEPS)

    @pl.when(is_top)
    def _():
        base = me[0] * NB
        for s in range(2):
            u = upper[pl.ds(base + s * height, height), :]
            for g in range(GROUPS):
                out[s, g] = u[:, g * LANES : (g + 1) * LANES]

    @pl.when(is_top & (me[1] < STEPS))
    def _():
        for s in range(2):
            for g in range(2):
                out[s, g] = final[me[0], me[1], s * height : (s + 1) * height, g * LANES : (g + 1) * LANES]

    for s in range(2):
        for g in range(GROUPS):
            done[s * height : (s + 1) * height, g, :] = out[s, g] + tiles[s * GROUPS + g]


def eliminate(me, linv, uinv, gathered, rows, tiles, chunks):
    parts, _, both, _ = gathered.shape
    height = rows.shape[0] // parts
    share = both - height
    width = GROUPS * LANES
    whole3 = pl.BlockSpec((STEPS, NB, NB), lambda i: (0, 0, 0))
    return pl.pallas_call(
        main_body,
        grid=(parts // 2,),
        in_specs=[
            SMEM,
            whole3,
            whole3,
            ANY,
            pl.BlockSpec((2, STEPS, height, NB), lambda i: (i, 0, 0, 0)),
            pl.BlockSpec((2 * height, GROUPS, LANES), lambda i: (i, 0, 0)),
            pl.BlockSpec((2 * GROUPS, height, LANES), lambda i: (i, 0, 0)),
        ]
        + [pl.BlockSpec(c.shape, lambda i: (0, 0, 0)) for c in chunks],
        out_specs=pl.BlockSpec((2 * height, GROUPS, LANES), lambda i: (i, 0, 0)),
        out_shape=jax.ShapeDtypeStruct(rows.shape, F32),
        scratch_shapes=[
            pltpu.VMEM((2, GROUPS, height, LANES), F32),
            pltpu.VMEM((STEPS * NB, GROUPS, LANES), F32),
            pltpu.VMEM((STEPS, STEPS, NB, NB), F32),
            pltpu.VMEM((STEPS * NB, width), F32),
            pltpu.VMEM((STEPS * NB, width), BF16),
            pltpu.VMEM((STEPS * NB, width), BF16),
            pltpu.VMEM((STEPS, NB, NB), F32),
            pltpu.VMEM((parts, STEPS, share, NB), F32),
            pltpu.SemaphoreType.DMA(()),
        ],
        compiler_params=room(42),
        name="eliminate",
    )(me, linv, uinv, gathered, gathered, rows, tiles, *chunks)


def sum_body(ids, received, out, acc, ring, order, ring_sem, out_sem):
    def note(i, n):
        order[n] = i
        return n + (ids[i] >= 0).astype(I32)

    total = lax.fori_loop(0, ids.shape[0], note, 0)

    def fetch(j):
        b = lax.rem(j, RING)
        return pltpu.make_async_copy(received.at[order[j]], ring.at[b], ring_sem.at[b])

    def prime(j, carry):
        fetch(j).start()
        return carry

    lax.fori_loop(0, jnp.minimum(total, RING), prime, 0)

    def clear(m, carry):
        acc[m] = jnp.zeros(acc.shape[1:], F32)
        return carry

    lax.fori_loop(0, acc.shape[0], clear, 0)

    def add(j, carry):
        fetch(j).wait()
        m = ids[order[j]]
        acc[m] = acc[m] + ring[lax.rem(j, RING)]

        @pl.when(j + RING < total)
        def _():
            fetch(j + RING).start()

        return carry

    lax.fori_loop(0, total, add, 0)
    copy = pltpu.make_async_copy(acc, out, out_sem)
    copy.start()
    copy.wait()


def sum_tiles(ids, received, spots):
    edge = received.shape[1]
    return pl.pallas_call(
        sum_body,
        in_specs=[SMEM, ANY],
        out_specs=ANY,
        out_shape=jax.ShapeDtypeStruct((spots, edge, LANES), F32),
        scratch_shapes=[
            pltpu.VMEM((spots, edge, LANES), F32),
            pltpu.VMEM((RING, edge, LANES), F32),
            pltpu.SMEM((ids.shape[0],), I32),
            pltpu.SemaphoreType.DMA((RING,)),
            pltpu.SemaphoreType.DMA(()),
        ],
        compiler_params=room(14),
        name="sum_tiles",
    )(ids, received)


def look(x, t, values, other):
    same = x[:, None] == t[None, :]
    hit = jnp.any(same, axis=1)
    return hit, jnp.where(hit, jnp.sum(jnp.where(same, values[None, :], 0), axis=1), other)


def permutation(swap_rows):
    t0, t1, t2 = swap_rows[0], swap_rows[1], swap_rows[2]
    j = jnp.arange(NB, dtype=I32)
    n = NB
    x = jnp.concatenate([NB + j, 2 * NB + j, t1, t2])
    _, once = look(x, t0, j, x)
    v1 = once[:n]
    y = jnp.concatenate([2 * NB + j, t2])
    _, twice = look(y, t1, v1, jnp.concatenate([once[n : 2 * n], once[3 * n :]]))
    v2 = twice[:n]
    source = jnp.concatenate([t0, once[2 * n : 3 * n], twice[n:]])
    below = STEPS * NB
    in1 = jnp.any(t0[:, None] == t1[None, :], axis=1)
    in2 = jnp.any(jnp.concatenate([t0, t1])[:, None] == t2[None, :], axis=1)
    ok0 = (t0 >= below) & ~in1 & ~in2[:n]
    ok1 = (t1 >= below) & ~in2[n:]
    ok2 = t2 >= below
    land = jnp.where(jnp.concatenate([ok0, ok1, ok2]), jnp.concatenate([t0, t1, t2]), -1)
    return source, land, jnp.concatenate([j, v1, v2])


def ranks(turn):
    i = jnp.arange(turn.shape[0], dtype=I32)
    earlier = (turn[:, None] == turn[None, :]) & (i[None, :] < i[:, None])
    return jnp.sum(earlier.astype(I32), axis=1)


def slots(turn, rank, cap, count, value):
    slot = jnp.where((turn >= 0) & (rank < cap), turn * cap + rank, -1)
    place = jnp.arange(count * cap, dtype=I32)
    same = slot[None, :] == place[:, None]
    return jnp.sum(jnp.where(same, value[None, :] + 1, 0), axis=1) - 1


def step(front_matrix, swap_rows, l_inverse, u_inverse, contrib_tiles, tile_owner, tile_spot):
    row_count = lax.axis_size("row")
    col_count = lax.axis_size("col")
    row_place = lax.axis_index("row").astype(I32)
    col_place = lax.axis_index("col").astype(I32)
    me = jnp.stack([row_place, col_place])
    local_rows = front_matrix.shape[0] * NB
    rows = front_matrix.reshape(-1).reshape(local_rows, GROUPS, LANES)

    def exchange(x, axes):
        return lax.all_to_all(x, axes, split_axis=0, concat_axis=0, tiled=True)

    def shift(x, t):
        return lax.ppermute(x, "row", [(p, (p + t) % row_count) for p in range(row_count)])

    def leave(x, t):
        return lax.ppermute(x, "row", [(p, (p + t) % row_count) for p in range(STEPS)])

    def home(x):
        block = x // NB
        here = (x >= 0) & (block % row_count == row_place)
        return jnp.where(here, block // row_count * NB + x % NB, -1)

    source, land, old = permutation(swap_rows)
    from_row = old // NB
    to_row = land // NB % row_count
    going = jnp.where((land >= 0) & (from_row == row_place), (to_row - row_place) % row_count, -1)
    coming = jnp.where((land >= 0) & (to_row == row_place), (row_place - from_row) % row_count, -1)
    pair = jnp.where(land >= 0, from_row * row_count + to_row, -1)
    loads = jnp.sum((pair[:, None] == jnp.arange(STEPS * row_count, dtype=I32)[None, :]).astype(I32), axis=0)

    owners = tile_owner[:, 0]
    slot = owners * CAP + jnp.minimum(ranks(owners), CAP - 1)
    total = row_count * col_count * CAP
    ids = slots(owners, slot - owners * CAP, CAP, row_count * col_count, tile_spot)
    leaving = slots(going, ranks(going), PARCEL, row_count, old % NB)
    landing = slots(coming, ranks(coming), PARCEL, row_count, home(land))
    picked = pick(me, leaving, home(source), rows, row_count)
    parcels, picked, corner = picked[:row_count], picked[row_count:-1], picked[-1]
    parcels = [parcels[0]] + [leave(parcels[t], t) for t in range(1, row_count)]
    given = [picked[0]] + [shift(picked[t], t) for t in range(1, row_count)]
    send = pack(contrib_tiles, slot, total)
    notes = ids.astype(F32).reshape(row_count, col_count, CAP).transpose(1, 0, 2).reshape(col_count, -1)
    notes = jnp.pad(notes[:, None, :], ((0, 0), (0, 7), (0, NB - notes.shape[1])))

    def ranked(parcels):
        return land_rows(landing, rows, corner, notes, parcels)

    def whole(parcels):
        every = [rows[:NB]] + [leave(rows[:NB], t) for t in range(1, row_count)]
        spread = slots(coming, old % NB, NB, row_count, home(land))
        return land_rows(spread, rows, corner, notes, every)

    parcels, landing = lax.optimization_barrier((parcels, landing))
    moved, parts = lax.cond(jnp.max(loads) > PARCEL, whole, ranked, parcels)
    dealt = exchange(parts, "col")
    tall = local_rows // col_count
    partial = dealt[:STEPS, tall:-8].reshape(-1, NB)
    notes = dealt[:, -8, : row_count * CAP].reshape(col_count, row_count, CAP).transpose(1, 0, 2)
    notes = jnp.pad(notes.reshape(1, -1), ((0, 7), (0, NB - notes.size)))
    partial = jnp.concatenate([partial, notes])
    partial = jnp.stack([partial] + [shift(partial, t) for t in range(1, row_count)])
    corner = jnp.sum(partial[:, :-8], axis=0).reshape(STEPS, -1, NB)
    mixed = jnp.concatenate([dealt[:STEPS, :tall], corner], axis=1)
    notes = partial[:, -8].reshape(row_count, -1)[:, : row_count * col_count * CAP]
    notes = lax.dynamic_slice_in_dim(notes, row_place * col_count * CAP, col_count * CAP, 1)
    turn = (row_place - jnp.arange(row_count, dtype=I32)) % row_count
    ids_in = notes[turn].reshape(-1).astype(I32)
    send, mixed, ids_in, *given = lax.optimization_barrier((send, mixed, ids_in, *given))
    received = exchange(send, ("row", "col"))
    received, mixed, *given = lax.optimization_barrier((received, mixed, *given))
    gathered = lax.all_gather(mixed.reshape(-1, NB), "col", axis=0, tiled=True)
    gathered = gathered.reshape(col_count, STEPS, -1, NB)
    summed = collect(given)
    chunks = [summed] + [shift(summed, t) for t in range(1, row_count)]
    tiles = sum_tiles(ids_in, received, local_rows // LANES * GROUPS)
    out = eliminate(me, l_inverse, u_inverse, gathered, moved, tiles, chunks)
    return out.reshape(-1).reshape(front_matrix.shape)


def solution(mesh):
    placed = (
        P(None, "row", None, None, "col", None),
        P(),
        P(),
        P(),
        P(("row", "col"), None, None),
        P(("row", "col"), None),
        P(("row", "col")),
    )
    return jax.shard_map(
        step,
        mesh=mesh,
        in_specs=placed,
        out_specs=P(None, "row", None, None, "col", None),
        check_vma=False,
    )
```

```python
import jax
import jax.numpy as jnp
from jax import lax
from jax.experimental import pallas as pl
from jax.experimental.pallas import tpu as pltpu
from jax.sharding import PartitionSpec as P


STEPS = 3
CAP = 2
NB = 256
LANES = 128
GROUPS = 8
RING = 16
PARCEL = 48
F32 = jnp.float32
BF16 = jnp.bfloat16
I32 = jnp.int32
ANY = pl.BlockSpec(memory_space=pl.ANY)
SMEM = pl.BlockSpec(memory_space=pltpu.SMEM)


def room(mib):
    return pltpu.CompilerParams(vmem_limit_bytes=mib * 1024 * 1024)


def halves(x):
    high = x.astype(BF16)
    return high, (x - high.astype(F32)).astype(BF16)


def product(a, b):
    def one(x, y):
        return jnp.dot(x, y, preferred_element_type=F32)

    return one(a[0], b[0]) + (one(a[0], b[1]) + one(a[1], b[0]))


def pack_body(slot, tiles, send, held, load_sem, sem):
    count = tiles.shape[0]
    load = pltpu.make_async_copy(tiles, held, load_sem)
    load.start()
    load.wait()

    def put(i, carry):
        pltpu.make_async_copy(held.at[i], send.at[slot[i]], sem).start()
        return carry

    lax.fori_loop(0, count, put, 0)
    pltpu.make_async_copy(held, send.at[pl.ds(0, count)], sem).wait()


def pack(tiles, slot, total):
    edge = tiles.shape[1]
    return pl.pallas_call(
        pack_body,
        in_specs=[SMEM, ANY],
        out_specs=ANY,
        out_shape=jax.ShapeDtypeStruct((total, edge, edge), F32),
        scratch_shapes=[
            pltpu.VMEM(tiles.shape, F32),
            pltpu.SemaphoreType.DMA(()),
            pltpu.SemaphoreType.DMA(()),
        ],
        compiler_params=room(60),
        name="pack_tiles",
    )(slot, tiles)


def pick_body(me, leaving, place, rows, *rest):
    count = (len(rest) - 4) // 2
    parcels, outs = rest[:count], rest[count : 2 * count]
    corner, held, sem, leave_sem = rest[2 * count :]
    cap = parcels[0].shape[0]
    share = outs[0].shape[0]
    sent = jnp.int32(0)
    for t in range(count):

        def fill(i, n, t=t):
            at = leaving[t * cap + i]

            @pl.when(at >= 0)
            def _():
                pltpu.make_async_copy(rows.at[at], parcels[t].at[i], leave_sem).start()

            return n + (at >= 0).astype(I32)

        sent = lax.fori_loop(0, cap, fill, sent)
    held[...] = jnp.zeros_like(held)

    def go(i, n):
        at = place[i]

        @pl.when(at >= 0)
        def _():
            pltpu.make_async_copy(rows.at[at], held.at[i], sem).start()

        return n + (at >= 0).astype(I32)

    started = lax.fori_loop(0, place.shape[0], go, 0)

    def finish(i, carry):
        pltpu.make_async_copy(rows.at[0], held.at[0], sem).wait()
        return carry

    def finish_leave(i, carry):
        pltpu.make_async_copy(rows.at[0], parcels[0].at[0], leave_sem).wait()
        return carry

    lax.fori_loop(0, sent, finish_leave, 0)
    lax.fori_loop(0, started, finish, 0)
    for g in range(2):
        corner[:, g * LANES : (g + 1) * LANES] = held[:, g, :]
    for t, out in enumerate(outs):
        out[...] = held[pl.ds(lax.rem(me[0] + t, count) * share, share)]


def pick(me, leaving, place, rows, count):
    total = place.shape[0]
    cap = leaving.shape[0] // count
    vmem = pl.BlockSpec(memory_space=pltpu.VMEM)
    return pl.pallas_call(
        pick_body,
        in_specs=[SMEM, SMEM, SMEM, ANY],
        out_specs=[vmem] * (2 * count + 1),
        out_shape=[jax.ShapeDtypeStruct((cap, GROUPS, LANES), F32)] * count
        + [jax.ShapeDtypeStruct((total // count, GROUPS, LANES), F32)] * count
        + [jax.ShapeDtypeStruct((total, NB), F32)],
        scratch_shapes=[
            pltpu.VMEM((total, GROUPS, LANES), F32),
            pltpu.SemaphoreType.DMA(()),
            pltpu.SemaphoreType.DMA(()),
        ],
        compiler_params=room(16),
        name="pick_rows",
    )(me, leaving, place, rows)


def collect_body(*refs):
    total = refs[0][...]
    for ref in refs[1:-1]:
        total = total + ref[...]
    refs[-1][...] = total


def collect(given):
    vmem = pl.BlockSpec(memory_space=pltpu.VMEM)
    return pl.pallas_call(
        collect_body,
        in_specs=[vmem] * len(given),
        out_specs=vmem,
        out_shape=jax.ShapeDtypeStruct(given[0].shape, F32),
        compiler_params=room(10),
        name="collect_rows",
    )(*given)


def land_body(landing, rows, corner, notes, *rest):
    parcels = rest[:-5]
    out, parts, held, sem, out_sem = rest[-5:]
    load = pltpu.make_async_copy(rows, held, sem)
    load.start()
    share = corner.shape[0] // parts.shape[0]
    height = held.shape[0] // parts.shape[0]

    def head(s, carry):
        parts[s, height : height + share] = corner[pl.ds(pl.multiple_of(s * share, 8), share)]
        parts[s, height + share :] = notes[s]
        return carry

    lax.fori_loop(0, parts.shape[0], head, 0)
    load.wait()
    for t, given in enumerate(parcels):
        cap = given.shape[0]

        def settle(i, carry, t=t, given=given, cap=cap):
            at = landing[t * cap + i]

            @pl.when(at >= 0)
            def _():
                held[at] = given[i]

            return carry

        lax.fori_loop(0, cap, settle, 0)
    save = pltpu.make_async_copy(held, out, out_sem)
    save.start()

    def body(s, carry):
        for g in range(2):
            parts[s, :height, g * LANES : (g + 1) * LANES] = held[pl.ds(s * height, height), g, :]
        return carry

    lax.fori_loop(0, parts.shape[0], body, 0)
    save.wait()


def land_rows(landing, rows, corner, notes, parcels):
    count = notes.shape[0]
    vmem = pl.BlockSpec(memory_space=pltpu.VMEM)
    length = rows.shape[0] // count + corner.shape[0] // count + notes.shape[1]
    return pl.pallas_call(
        land_body,
        in_specs=[SMEM, ANY, vmem, vmem] + [vmem] * len(parcels),
        out_specs=[ANY, vmem],
        out_shape=[
            jax.ShapeDtypeStruct(rows.shape, F32),
            jax.ShapeDtypeStruct((count, length, NB), F32),
        ],
        scratch_shapes=[
            pltpu.VMEM(rows.shape, F32),
            pltpu.SemaphoreType.DMA(()),
            pltpu.SemaphoreType.DMA(()),
        ],
        compiler_params=room(28),
    )(landing, rows, corner, notes, *parcels)


def main_body(me, linv, uinv, gathered, panels, block, tiles, *rest):
    chunks = rest[:-10]
    done, out, chosen, final, upper, upper_hi, upper_lo, factor, corner, sem = rest[-10:]
    step = pl.program_id(0)
    height = panels.shape[2]

    def ui(k):
        return halves(uinv[k])

    @pl.when(step == 0)
    def _():
        copy = pltpu.make_async_copy(gathered.at[:, :, pl.ds(height, corner.shape[2]), :], corner, sem)
        copy.start()
        for t, chunk in enumerate(chunks):
            share = chunk.shape[0]
            chosen[pl.ds(lax.rem(me[0] - t + len(chunks), len(chunks)) * share, share)] = chunk[...]
        copy.wait()
        cols = [corner[:, k].reshape(STEPS * NB, NB) for k in range(STEPS)]
        n = [[cols[k][i * NB : (i + 1) * NB] for k in range(STEPS)] for i in range(STEPS)]
        low = {}
        for k in range(STEPS):
            x = chosen[k * NB : (k + 1) * NB].reshape(NB, GROUPS * LANES)
            for m in range(k):
                x = x - product(low[k, m], (upper_hi[m * NB : (m + 1) * NB], upper_lo[m * NB : (m + 1) * NB]))
            u = product(halves(linv[k]), halves(x))
            hi, lo = halves(u)
            upper[k * NB : (k + 1) * NB] = u
            upper_hi[k * NB : (k + 1) * NB] = hi
            upper_lo[k * NB : (k + 1) * NB] = lo
            final[k, k] = n[k][k]
            for i in range(k + 1, STEPS):
                l = product(halves(n[i][k]), ui(k))
                low[i, k] = halves(l)
                final[i, k] = l
                v = product(halves(linv[k]), halves(n[k][i]))
                final[k, i] = v
            for i in range(k + 1, STEPS):
                for j in range(k + 1, STEPS):
                    n[i][j] = n[i][j] - product(low[i, k], halves(final[k, j]))

    hi = []
    lo = []
    for k in range(STEPS):
        x = panels[:, k].reshape(2 * height, NB)
        for m in range(k):
            x = x - product((hi[m], lo[m]), halves(final[m, k]))
        l = product(halves(x), ui(k))
        factor[k] = l
        h, w = halves(l)
        hi.append(h)
        lo.append(w)
    high = jnp.concatenate(hi, axis=1)
    rest = jnp.concatenate(lo, axis=1)
    update = product((high, rest), (upper_hi[...], upper_lo[...]))
    value = block[...].reshape(2 * height, GROUPS * LANES) - update
    for s in range(2):
        for g in range(GROUPS):
            out[s, g] = value[s * height : (s + 1) * height, g * LANES : (g + 1) * LANES]

    @pl.when(me[1] < STEPS)
    def _():
        for s in range(2):
            for g in range(2):
                out[s, g] = factor[me[1], s * height : (s + 1) * height, g * LANES : (g + 1) * LANES]

    is_top = (step == 0) & (me[0] < STEPS)

    @pl.when(is_top)
    def _():
        base = me[0] * NB
        for s in range(2):
            u = upper[pl.ds(base + s * height, height), :]
            for g in range(GROUPS):
                out[s, g] = u[:, g * LANES : (g + 1) * LANES]

    @pl.when(is_top & (me[1] < STEPS))
    def _():
        for s in range(2):
            for g in range(2):
                out[s, g] = final[me[0], me[1], s * height : (s + 1) * height, g * LANES : (g + 1) * LANES]

    for s in range(2):
        for g in range(GROUPS):
            done[s * height : (s + 1) * height, g, :] = out[s, g] + tiles[s * GROUPS + g]


def eliminate(me, linv, uinv, gathered, rows, tiles, chunks):
    parts, _, both, _ = gathered.shape
    height = rows.shape[0] // parts
    share = both - height
    width = GROUPS * LANES
    whole3 = pl.BlockSpec((STEPS, NB, NB), lambda i: (0, 0, 0))
    return pl.pallas_call(
        main_body,
        grid=(parts // 2,),
        in_specs=[
            SMEM,
            whole3,
            whole3,
            ANY,
            pl.BlockSpec((2, STEPS, height, NB), lambda i: (i, 0, 0, 0)),
            pl.BlockSpec((2 * height, GROUPS, LANES), lambda i: (i, 0, 0)),
            pl.BlockSpec((2 * GROUPS, height, LANES), lambda i: (i, 0, 0)),
        ]
        + [pl.BlockSpec(c.shape, lambda i: (0, 0, 0)) for c in chunks],
        out_specs=pl.BlockSpec((2 * height, GROUPS, LANES), lambda i: (i, 0, 0)),
        out_shape=jax.ShapeDtypeStruct(rows.shape, F32),
        scratch_shapes=[
            pltpu.VMEM((2, GROUPS, height, LANES), F32),
            pltpu.VMEM((STEPS * NB, GROUPS, LANES), F32),
            pltpu.VMEM((STEPS, STEPS, NB, NB), F32),
            pltpu.VMEM((STEPS * NB, width), F32),
            pltpu.VMEM((STEPS * NB, width), BF16),
            pltpu.VMEM((STEPS * NB, width), BF16),
            pltpu.VMEM((STEPS, NB, NB), F32),
            pltpu.VMEM((parts, STEPS, share, NB), F32),
            pltpu.SemaphoreType.DMA(()),
        ],
        compiler_params=room(42),
        name="eliminate",
    )(me, linv, uinv, gathered, gathered, rows, tiles, *chunks)


def sum_body(ids, received, out, acc, ring, order, ring_sem, out_sem):
    def note(i, n):
        order[n] = i
        return n + (ids[i] >= 0).astype(I32)

    total = lax.fori_loop(0, ids.shape[0], note, 0)

    def fetch(j):
        b = lax.rem(j, RING)
        return pltpu.make_async_copy(received.at[order[j]], ring.at[b], ring_sem.at[b])

    def prime(j, carry):
        fetch(j).start()
        return carry

    lax.fori_loop(0, jnp.minimum(total, RING), prime, 0)

    def clear(m, carry):
        acc[m] = jnp.zeros(acc.shape[1:], F32)
        return carry

    lax.fori_loop(0, acc.shape[0], clear, 0)

    def add(j, carry):
        fetch(j).wait()
        m = ids[order[j]]
        acc[m] = acc[m] + ring[lax.rem(j, RING)]

        @pl.when(j + RING < total)
        def _():
            fetch(j + RING).start()

        return carry

    lax.fori_loop(0, total, add, 0)
    copy = pltpu.make_async_copy(acc, out, out_sem)
    copy.start()
    copy.wait()


def sum_tiles(ids, received, spots):
    edge = received.shape[1]
    return pl.pallas_call(
        sum_body,
        in_specs=[SMEM, ANY],
        out_specs=ANY,
        out_shape=jax.ShapeDtypeStruct((spots, edge, LANES), F32),
        scratch_shapes=[
            pltpu.VMEM((spots, edge, LANES), F32),
            pltpu.VMEM((RING, edge, LANES), F32),
            pltpu.SMEM((ids.shape[0],), I32),
            pltpu.SemaphoreType.DMA((RING,)),
            pltpu.SemaphoreType.DMA(()),
        ],
        compiler_params=room(60),
        name="sum_tiles",
    )(ids, received)


def look(x, t, values, other):
    same = x[:, None] == t[None, :]
    hit = jnp.any(same, axis=1)
    return hit, jnp.where(hit, jnp.sum(jnp.where(same, values[None, :], 0), axis=1), other)


def permutation(swap_rows):
    t0, t1, t2 = swap_rows[0], swap_rows[1], swap_rows[2]
    j = jnp.arange(NB, dtype=I32)
    n = NB
    x = jnp.concatenate([NB + j, 2 * NB + j, t1, t2])
    _, once = look(x, t0, j, x)
    v1 = once[:n]
    y = jnp.concatenate([2 * NB + j, t2])
    _, twice = look(y, t1, v1, jnp.concatenate([once[n : 2 * n], once[3 * n :]]))
    v2 = twice[:n]
    source = jnp.concatenate([t0, once[2 * n : 3 * n], twice[n:]])
    below = STEPS * NB
    in1 = jnp.any(t0[:, None] == t1[None, :], axis=1)
    in2 = jnp.any(jnp.concatenate([t0, t1])[:, None] == t2[None, :], axis=1)
    ok0 = (t0 >= below) & ~in1 & ~in2[:n]
    ok1 = (t1 >= below) & ~in2[n:]
    ok2 = t2 >= below
    land = jnp.where(jnp.concatenate([ok0, ok1, ok2]), jnp.concatenate([t0, t1, t2]), -1)
    return source, land, jnp.concatenate([j, v1, v2])


def ranks(turn):
    i = jnp.arange(turn.shape[0], dtype=I32)
    earlier = (turn[:, None] == turn[None, :]) & (i[None, :] < i[:, None])
    return jnp.sum(earlier.astype(I32), axis=1)


def slots(turn, rank, cap, count, value):
    slot = jnp.where((turn >= 0) & (rank < cap), turn * cap + rank, -1)
    place = jnp.arange(count * cap, dtype=I32)
    same = slot[None, :] == place[:, None]
    return jnp.sum(jnp.where(same, value[None, :] + 1, 0), axis=1) - 1


def step(front_matrix, swap_rows, l_inverse, u_inverse, contrib_tiles, tile_owner, tile_spot):
    row_count = lax.axis_size("row")
    col_count = lax.axis_size("col")
    row_place = lax.axis_index("row").astype(I32)
    col_place = lax.axis_index("col").astype(I32)
    me = jnp.stack([row_place, col_place])
    local_rows = front_matrix.shape[0] * NB
    rows = front_matrix.reshape(-1).reshape(local_rows, GROUPS, LANES)

    def exchange(x, axes):
        return lax.all_to_all(x, axes, split_axis=0, concat_axis=0, tiled=True)

    def shift(x, t):
        return lax.ppermute(x, "row", [(p, (p + t) % row_count) for p in range(row_count)])

    def leave(x, t):
        return lax.ppermute(x, "row", [(p, (p + t) % row_count) for p in range(STEPS)])

    def home(x):
        block = x // NB
        here = (x >= 0) & (block % row_count == row_place)
        return jnp.where(here, block // row_count * NB + x % NB, -1)

    source, land, old = permutation(swap_rows)
    from_row = old // NB
    to_row = land // NB % row_count
    going = jnp.where((land >= 0) & (from_row == row_place), (to_row - row_place) % row_count, -1)
    coming = jnp.where((land >= 0) & (to_row == row_place), (row_place - from_row) % row_count, -1)
    pair = jnp.where(land >= 0, from_row * row_count + to_row, -1)
    loads = jnp.sum((pair[:, None] == jnp.arange(STEPS * row_count, dtype=I32)[None, :]).astype(I32), axis=0)

    owners = tile_owner[:, 0]
    slot = owners * CAP + jnp.minimum(ranks(owners), CAP - 1)
    total = row_count * col_count * CAP
    ids = slots(owners, slot - owners * CAP, CAP, row_count * col_count, tile_spot)
    leaving = slots(going, ranks(going), PARCEL, row_count, old % NB)
    landing = slots(coming, ranks(coming), PARCEL, row_count, home(land))
    picked = pick(me, leaving, home(source), rows, row_count)
    parcels, picked, corner = picked[:row_count], picked[row_count:-1], picked[-1]
    parcels = [parcels[0]] + [leave(parcels[t], t) for t in range(1, row_count)]
    given = [picked[0]] + [shift(picked[t], t) for t in range(1, row_count)]
    send = pack(contrib_tiles, slot, total)
    notes = ids.astype(F32).reshape(row_count, col_count, CAP).transpose(1, 0, 2).reshape(col_count, -1)
    notes = jnp.pad(notes[:, None, :], ((0, 0), (0, 7), (0, NB - notes.shape[1])))

    def ranked(parcels):
        return land_rows(landing, rows, corner, notes, parcels)

    def whole(parcels):
        every = [rows[:NB]] + [leave(rows[:NB], t) for t in range(1, row_count)]
        spread = slots(coming, old % NB, NB, row_count, home(land))
        return land_rows(spread, rows, corner, notes, every)

    parcels, landing = lax.optimization_barrier((parcels, landing))
    moved, parts = lax.cond(jnp.max(loads) > PARCEL, whole, ranked, parcels)
    dealt = exchange(parts, "col")
    tall = local_rows // col_count
    partial = dealt[:STEPS, tall:-8].reshape(-1, NB)
    notes = dealt[:, -8, : row_count * CAP].reshape(col_count, row_count, CAP).transpose(1, 0, 2)
    notes = jnp.pad(notes.reshape(1, -1), ((0, 7), (0, NB - notes.size)))
    partial = jnp.concatenate([partial, notes])
    summed = collect(given)
    chunks = [summed] + [shift(summed, t) for t in range(1, row_count)]
    partial = jnp.stack([partial] + [shift(partial, t) for t in range(1, row_count)])
    corner = jnp.sum(partial[:, :-8], axis=0).reshape(STEPS, -1, NB)
    mixed = jnp.concatenate([dealt[:STEPS, :tall], corner], axis=1)
    notes = partial[:, -8].reshape(row_count, -1)[:, : row_count * col_count * CAP]
    notes = lax.dynamic_slice_in_dim(notes, row_place * col_count * CAP, col_count * CAP, 1)
    turn = (row_place - jnp.arange(row_count, dtype=I32)) % row_count
    ids_in = notes[turn].reshape(-1).astype(I32)
    send, mixed, ids_in, *chunks = lax.optimization_barrier((send, mixed, ids_in, *chunks))
    received = exchange(send, ("row", "col"))
    received, mixed = lax.optimization_barrier((received, mixed))
    gathered = lax.all_gather(mixed.reshape(-1, NB), "col", axis=0, tiled=True)
    gathered = gathered.reshape(col_count, STEPS, -1, NB)
    tiles = sum_tiles(ids_in, received, local_rows // LANES * GROUPS)
    out = eliminate(me, l_inverse, u_inverse, gathered, moved, tiles, chunks)
    return out.reshape(-1).reshape(front_matrix.shape)


def solution(mesh):
    placed = (
        P(None, "row", None, None, "col", None),
        P(),
        P(),
        P(),
        P(("row", "col"), None, None),
        P(("row", "col"), None),
        P(("row", "col")),
    )
    return jax.shard_map(
        step,
        mesh=mesh,
        in_specs=placed,
        out_specs=P(None, "row", None, None, "col", None),
        check_vma=False,
    )
```
